256 devices in a mesh: groups: 2 (over z), ctx: 128 (over y, x, core).
Axes of the slice: x: 8, y: 8, z: 2, core: 2. Of those that a mesh axis runs over, the one named last changes fastest.
The devices are a block of a 8x8x16 slice.
Arguments:
- query_states: bfloat16 [131072, 32, 128], P(('groups', 'ctx')), parts along dimension 0, may hold values from -20 to 20
- key_states: bfloat16 [131072, 8, 128], P(('groups', 'ctx')), parts along dimension 0, may hold values from -4 to 4
- value_states: bfloat16 [131072, 8, 128], P(('groups', 'ctx')), parts along dimension 0, may hold values from -6 to 6
- vert_blocks: int32 [16, 4], P('groups'), parts along dimension 0, may hold values from 0 to 511, as said below
- vert_count: int32 [16], P('groups'), parts along dimension 0, may hold values from 1 to 4, as said below
- slash_offsets: int32 [16, 4], P('groups'), parts along dimension 0, may hold values from 0 to 8, as said below
- slash_count: int32 [16], P('groups'), parts along dimension 0, may hold values from 1 to 4, as said below
Outputs:
- attended: bfloat16 [131072, 32, 128], P(('groups', 'ctx')), parts along dimension 0
The draws below stay inside these ranges and needn't reach their ends.
There are 2 independent parts, one for each index of `groups`. The reference program is written for one: setup_inputs(seed, part) draws one part's arguments, and reference() takes and returns one part's arrays. A program takes and returns all parts, laid end to end along the dimension named above; each array names one. Nothing has to cross between parts.
Inputs may be any that keep to these rules, and one draw needn't show every extreme that they name: `vert_blocks`: the 4 entries of each head are distinct; in some head the first entry lies in one of the first 4 blocks. `vert_count`: some head uses all 4 entries. `slash_offsets`: the 4 entries of each head are distinct and the first is 0. `slash_count`: some head uses all 4 entries.
All inputs are finite; a program needn't handle non-finite values.
Results may differ from the reference program's by a relative error of at most 0.0048.
Values may be sent and summed in bfloat16 or wider, within the bound.
No kernel may reach another device: no remote copies, remote signals or barrier semaphores. Data moves between devices by JAX's collectives and lax.ppermute only.
A program may use at most 128 MiB of HBM per device.

```python
import math
import jax
import jax.numpy as jnp
from jax import lax

QH = 32
KVH = 8
DH = 128
BLOCK = 128
NV = 4
NS = 4
SEQ_DEV = 512
TOKENS = 65536
NBLK = 512


def draw_query_states(key, part):
    base = jnp.clip(jax.random.normal(jax.random.fold_in(key, 11), (TOKENS, QH, DH), jnp.float32), -4.0, 4.0)
    return base.astype(jnp.bfloat16)


def draw_key_states(key, part):
    base = jnp.clip(jax.random.normal(jax.random.fold_in(key, 12), (TOKENS, KVH, DH), jnp.float32), -4.0, 4.0)
    return base.astype(jnp.bfloat16)


def draw_vert_blocks(key, part):
    head_keys = jax.random.split(jax.random.fold_in(key, 21), KVH)
    picked = jax.vmap(lambda one_key: jax.random.permutation(one_key, NBLK)[:NV])(head_keys).astype(jnp.int32)
    first_dev = SEQ_DEV // BLOCK
    lowest = jax.random.randint(jax.random.fold_in(key, 22), (), 0, first_dev).astype(jnp.int32)
    others = jax.random.permutation(jax.random.fold_in(key, 23), NBLK - 1)[:NV - 1].astype(jnp.int32)
    others = others + (others >= lowest).astype(jnp.int32)
    special = jnp.concatenate((lowest[None], others))
    chosen = jax.random.randint(jax.random.fold_in(key, 24), (), 0, KVH)
    picked = jnp.where((jnp.arange(KVH) == chosen)[:, None], special[None, :], picked)
    return picked.astype(jnp.int32)


def draw_vert_count(key, part):
    counts = jax.random.randint(jax.random.fold_in(key, 31), (KVH,), 1, NV + 1)
    fullest = jax.random.randint(jax.random.fold_in(key, 32), (), 0, KVH)
    return counts.at[fullest].set(NV).astype(jnp.int32)


def draw_slash_offsets(key, part):
    head_keys = jax.random.split(jax.random.fold_in(key, 41), KVH)
    reach = 2 * (SEQ_DEV // BLOCK)
    others = jax.vmap(lambda one_key: jax.random.permutation(one_key, reach)[:NS - 1] + 1)(head_keys)
    return jnp.concatenate((jnp.zeros((KVH, 1), jnp.int32), others.astype(jnp.int32)), axis=1)


def draw_slash_count(key, part):
    counts = jax.random.randint(jax.random.fold_in(key, 51), (KVH,), 1, NS + 1)
    fullest = jax.random.randint(jax.random.fold_in(key, 52), (), 0, KVH)
    return counts.at[fullest].set(NS).astype(jnp.int32)


def block_scale(rng, shape, cuts, low, largest):
    def one(position, blocks):
        draws = jax.random.uniform(jax.random.fold_in(jax.random.fold_in(rng, 6), position), (blocks,), jnp.float32, low / len(cuts), largest / len(cuts))
        return jnp.repeat(jnp.exp(draws), shape[position] // blocks).reshape((-1,) + (1,) * (len(shape) - position - 1))

    gain = one(*cuts[0])
    for cut in cuts[1:]:
        gain = gain * one(*cut)
    return gain


def centred(key, dims, deviation, bound, pieces=(), kind=jnp.bfloat16):
    entries = deviation * jax.random.normal(key, dims, jnp.float32)
    if pieces:
        entries = entries * block_scale(key, dims, pieces, -0.22, 0.18)
    return jnp.clip(entries, -bound, bound).astype(kind)


def setup_inputs(seed: int = 0, part: int = 0) -> dict:
    key_of = jax.random.split(jax.random.key(seed), 8)
    part_keys = jax.random.split(jax.random.fold_in(key_of[7], part), 8)
    query_states = draw_query_states(jax.random.fold_in(jax.random.fold_in(key_of[7], part), 71), part)
    key_states = draw_key_states(jax.random.fold_in(jax.random.fold_in(key_of[7], part), 71), part)
    value_states = centred(part_keys[2], (TOKENS, KVH, DH), 1.0, 6.0, ((0, 128),))
    vert_blocks = draw_vert_blocks(jax.random.fold_in(jax.random.fold_in(key_of[7], part), 71), part)
    vert_count = draw_vert_count(jax.random.fold_in(jax.random.fold_in(key_of[7], part), 71), part)
    slash_offsets = draw_slash_offsets(jax.random.fold_in(jax.random.fold_in(key_of[7], part), 71), part)
    slash_count = draw_slash_count(jax.random.fold_in(jax.random.fold_in(key_of[7], part), 71), part)
    return dict(query_states=query_states, key_states=key_states, value_states=value_states, vert_blocks=vert_blocks, vert_count=vert_count, slash_offsets=slash_offsets, slash_count=slash_count)


def reference(query_states, key_states, value_states, vert_blocks, vert_count, slash_offsets, slash_count):
    group_size = QH // KVH
    key_tiles_all = key_states.reshape(NBLK, BLOCK, KVH, DH)
    value_tiles_all = value_states.reshape(NBLK, BLOCK, KVH, DH)
    head_ids = jnp.arange(KVH, dtype=jnp.int32)
    vert_slot = jnp.arange(NV, dtype=jnp.int32)[None, :] < vert_count[:, None]
    slash_slot = jnp.arange(NS, dtype=jnp.int32)[None, :] < slash_count[:, None]
    inv_root = 1.0 / math.sqrt(DH)
    within = jnp.arange(BLOCK, dtype=jnp.int32)

    def query_block(qblock):
        slash_blocks = qblock - slash_offsets
        repeated = jnp.any(vert_slot[:, None, :] & (vert_blocks[:, None, :] == slash_blocks[:, :, None]), axis=-1)
        slash_ok = slash_slot & (slash_blocks >= 0) & jnp.logical_not(repeated)
        vert_ok = vert_slot & (vert_blocks <= qblock)
        key_blocks = jnp.concatenate((vert_blocks, slash_blocks), axis=1)
        usable = jnp.concatenate((vert_ok, slash_ok), axis=1)
        clipped = jnp.clip(key_blocks, 0, NBLK - 1)
        key_tiles = key_tiles_all[clipped, :, head_ids[:, None], :]
        value_tiles = value_tiles_all[clipped, :, head_ids[:, None], :]
        query_rows = lax.dynamic_slice_in_dim(query_states, qblock * BLOCK, BLOCK, 0).reshape(BLOCK, KVH, group_size, DH)
        scores = jnp.einsum('qgrd,gntd->grqnt', query_rows.astype(jnp.float32), key_tiles.astype(jnp.float32)) * inv_root
        scores = scores.reshape(KVH, group_size, BLOCK, (NV + NS) * BLOCK)
        key_pos = (key_blocks[:, :, None] * BLOCK + within[None, None, :]).reshape(KVH, (NV + NS) * BLOCK)
        query_pos = qblock * BLOCK + within
        allowed = jnp.repeat(usable, BLOCK, axis=1)[:, None, :] & (key_pos[:, None, :] <= query_pos[None, :, None])
        allowed = allowed[:, None, :, :]
        masked = jnp.where(allowed, scores, -1e+30)
        row_max = lax.optimization_barrier(jnp.max(masked, axis=-1, keepdims=True))
        powers = jnp.where(allowed, jnp.exp(masked - row_max), 0.0)
        weights = (powers / lax.optimization_barrier(jnp.sum(powers, axis=-1, keepdims=True))).astype(jnp.bfloat16)
        values_flat = value_tiles.reshape(KVH, (NV + NS) * BLOCK, DH).astype(jnp.float32)
        result = jnp.einsum('grqk,gkd->qgrd', weights.astype(jnp.float32), values_flat)
        return result.reshape(BLOCK, QH, DH).astype(jnp.bfloat16)
    blocks = lax.map(query_block, jnp.arange(NBLK, dtype=jnp.int32))
    return blocks.reshape(TOKENS, QH, DH)
```

```python
import functools
import math

import jax
import jax.numpy as jnp
from jax import lax
from jax.experimental import pallas as pl
from jax.experimental.pallas import tpu as pltpu
from jax.sharding import PartitionSpec as P

BLOCK = 128
PIECE = 8


def shifted(x, axis, by):
    size = lax.axis_size(axis)
    pairs = [(i, i + by) for i in range(size) if 0 <= i + by < size]
    return lax.ppermute(x, axis, pairs)


def to_partner(x, axis, parity):
    size = lax.axis_size(axis)
    pairs = [(i, i ^ 1) for i in range(size) if i % 2 == parity]
    return lax.ppermute(x, axis, pairs)


def vertical_tables(vert_blocks, vert_count, per_dev, size, slots):
    heads, n_vert = vert_blocks.shape
    used = (jnp.arange(n_vert)[None, :] < vert_count[:, None]).reshape(-1)
    flat = vert_blocks.reshape(-1)
    owner = jnp.where(used, flat // per_dev, size)
    order = jnp.arange(heads * n_vert)
    same = (owner[None, :] == owner[:, None]) & (order[None, :] < order[:, None])
    within = jnp.sum(same, axis=1, dtype=jnp.int32)
    rank = within + jnp.sum(owner[None, :] < owner[:, None], axis=1, dtype=jnp.int32)
    turn = within // slots
    turns = jnp.max(jnp.where(used, turn, 0)) + 1
    tile = (order // n_vert) * per_dev + flat % per_dev
    return owner, rank, turn, turns, tile


def spread_vertical(pool, tables, device, axis):
    owner, rank, turn, turns, tile = tables
    size = lax.axis_size(axis)
    tiles, rows, width = pool.shape
    pieces = rows // PIECE
    slots = size // pieces
    each = len(owner) // slots
    slot = rank % slots
    mine = device // pieces
    of_j = (rank[None, :] == jnp.arange(each)[:, None] * slots + mine).astype(jnp.int32)
    from_j = jnp.clip(jnp.sum(of_j * owner[None, :], axis=1), 0, size - 1)
    turn_j = jnp.sum(of_j * turn[None, :], axis=1)

    def exchange(t, kept):
        here = (owner == device) & (turn == t)
        pick = jnp.sum(
            (here[None, :] & (slot[None, :] == jnp.arange(slots)[:, None])) * tile[None, :], axis=1
        )
        send = jnp.concatenate(
            [lax.dynamic_slice_in_dim(pool, pick[i], 1, 0) for i in range(slots)], axis=0
        )
        got = lax.all_to_all(send.reshape(size, PIECE, width), axis, 0, 0, tiled=True)
        new = jnp.concatenate(
            [lax.dynamic_slice_in_dim(got, from_j[j], 1, 0) for j in range(each)], axis=0
        )
        return jnp.where((turn_j == t)[:, None, None], new, kept)

    first = exchange(0, jnp.zeros((each, PIECE, width), pool.dtype))
    held = lax.while_loop(
        lambda c: c[0] < turns, lambda c: (c[0] + 1, exchange(c[0], c[1])), (jnp.int32(1), first)
    )[1]
    whole = lax.all_gather(held.reshape(each * PIECE, width), axis, tiled=True)
    return whole.reshape(slots, pieces, each, PIECE, width)


def tile_lists(vert_blocks, vert_count, slash_offsets, slash_count, device, per_dev):
    heads, n_vert = vert_blocks.shape
    n_slash = slash_offsets.shape[1]
    local_ids = jnp.arange(per_dev, dtype=jnp.int32)
    qblock = device * per_dev + local_ids
    vert_slot = jnp.arange(n_vert)[None, :] < vert_count[:, None]
    vert_ok = vert_slot[:, None, :] & (vert_blocks[:, None, :] < qblock[None, :, None])
    vert_at = jnp.broadcast_to(3 * per_dev + jnp.arange(n_vert), vert_ok.shape)
    slash_blocks = qblock[None, :, None] - slash_offsets[:, None, :]
    repeated = jnp.any(
        vert_slot[:, None, None, :] & (vert_blocks[:, None, None, :] == slash_blocks[..., None]),
        axis=-1,
    )
    slash_ok = (
        (jnp.arange(n_slash)[None, :] < slash_count[:, None])[:, None, :]
        & (slash_offsets > 0)[:, None, :]
        & (slash_blocks >= 0)
        & jnp.logical_not(repeated)
    )
    slash_at = local_ids[None, :, None] - slash_offsets[:, None, :] + 2 * per_dev
    ok = jnp.concatenate((slash_ok, vert_ok), axis=-1)
    at = jnp.concatenate((slash_at, vert_at), axis=-1).astype(jnp.int32)
    width = n_vert + n_slash
    earlier = jnp.arange(width)[None, :] < jnp.arange(width)[:, None]
    place = jnp.sum(ok[..., None, :] & earlier, axis=-1, dtype=jnp.int32) + 1
    hit = ok[..., None, :] & (place[..., None, :] == jnp.arange(1, width)[:, None])
    chosen = jnp.sum(jnp.where(hit, at[..., None, :], 0), axis=-1, dtype=jnp.int32)
    count = jnp.sum(ok, axis=-1, dtype=jnp.int32)[..., None] + 1
    return jnp.concatenate((count, chosen), axis=-1).reshape(heads * per_dev, width)


def attend_body(
    lists, spots, core, q_ref, own_ref, core_ref, chip_ref, far_ref, vert_ref, out_ref,
    keys, vals, scores, *, n_vert, per_dev, most
):
    head = pl.program_id(0)
    group = q_ref.shape[1]
    scale = math.log2(math.e) / math.sqrt(q_ref.shape[-1])

    def put(at, tile):
        keys[at] = tile[:BLOCK]
        vals[at] = tile[BLOCK:]

    for i in range(per_dev):
        put(i, far_ref[0, i])
        put(2 * per_dev + i, own_ref[0, i])

    @pl.when(core[0] == 1)
    def _():
        for i in range(per_dev):
            put(per_dev + i, core_ref[0, i])

    @pl.when(core[0] == 0)
    def _():
        for i in range(per_dev):
            put(per_dev + i, chip_ref[0, i])

    for i in range(n_vert):
        slot = spots[2 * (head * n_vert + i)]
        j = spots[2 * (head * n_vert + i) + 1]
        put(3 * per_dev + i, vert_ref[slot, :, j].reshape(2 * BLOCK, BLOCK))

    row = lax.broadcasted_iota(jnp.int32, (BLOCK, BLOCK), 0)
    col = lax.broadcasted_iota(jnp.int32, (BLOCK, BLOCK), 1)
    ones = jnp.ones((2 * BLOCK, BLOCK), jnp.bfloat16)

    def block(l, carry):
        line = head * per_dev + l
        count = lists[line, 0]

        def run(n):
            at = [2 * per_dev + l] + [lists[line, i] for i in range(1, n)]
            parts = [at[i : i + 2] for i in range(0, n, 2)]
            for r in range(group):
                q = q_ref[0, r, pl.ds(l * BLOCK, BLOCK), :]
                top = None
                for c, part in enumerate(parts):
                    k = jnp.concatenate([keys[i] for i in part], axis=0)
                    s = lax.dot_general(
                        q, k, (((1,), (1,)), ((), ())), preferred_element_type=jnp.float32
                    )
                    halves = [s[:, i * BLOCK : (i + 1) * BLOCK] for i in range(len(part))]
                    if c == 0:
                        halves[0] = jnp.where(col <= row, halves[0], -jnp.inf)
                    for i, half in enumerate(halves):
                        half = half * scale
                        scores[r, :, pl.ds((2 * c + i) * BLOCK, BLOCK)] = half
                        top = half if top is None else jnp.maximum(top, half)
                top = jnp.max(top, axis=-1, keepdims=True)
                acc = None
                for c, part in enumerate(parts):
                    wide = len(part) * BLOCK
                    p = jnp.exp2(scores[r, :, pl.ds(2 * c * BLOCK, wide)] - top)
                    v = jnp.concatenate([vals[i] for i in part], axis=0)
                    v = jnp.concatenate([v, ones[:wide]], axis=1)
                    o = jnp.dot(p.astype(jnp.bfloat16), v, preferred_element_type=jnp.float32)
                    acc = o if acc is None else acc + o
                out_ref[0, r, pl.ds(l * BLOCK, BLOCK), :] = (
                    acc[:, :BLOCK] / acc[:, BLOCK:]
                ).astype(out_ref.dtype)

        for n in range(1, most + 1):
            pl.when(count == n)(functools.partial(run, n))
        return carry

    lax.fori_loop(0, per_dev, block, 0)


def attend(queries, own, core_kv, chip_kv, far, vert, lists, spots, core):
    heads, group, rows, dim = queries.shape
    per_dev = own.shape[1]
    n_vert = len(spots) // 2 // heads
    most = lists.shape[1]
    by_head = lambda h, *_: (h, 0, 0, 0)
    kv_spec = pl.BlockSpec((1, *own.shape[1:]), by_head)
    q_spec = pl.BlockSpec((1, group, rows, dim), by_head)
    return pl.pallas_call(
        functools.partial(attend_body, n_vert=n_vert, per_dev=per_dev, most=most),
        grid_spec=pltpu.PrefetchScalarGridSpec(
            num_scalar_prefetch=3,
            grid=(heads,),
            in_specs=[
                q_spec, kv_spec, kv_spec, kv_spec, kv_spec,
                pl.BlockSpec(vert.shape, lambda h, *_: (0,) * vert.ndim),
            ],
            out_specs=q_spec,
            scratch_shapes=[
                pltpu.VMEM((3 * per_dev + n_vert, BLOCK, dim), own.dtype),
                pltpu.VMEM((3 * per_dev + n_vert, BLOCK, dim), own.dtype),
                pltpu.VMEM((group, BLOCK, most * BLOCK), jnp.float32),
            ],
        ),
        out_shape=jax.ShapeDtypeStruct(queries.shape, queries.dtype),
        name="attend",
    )(lists, spots, core, queries, own, core_kv, chip_kv, far, vert)


def local(
    query_states, key_states, value_states, vert_blocks, vert_count, slash_offsets, slash_count
):
    rows_dev, q_heads, head_dim = query_states.shape
    kv_heads = key_states.shape[1]
    group_size = q_heads // kv_heads
    per_dev = rows_dev // BLOCK
    n_vert = vert_blocks.shape[1]
    size = lax.axis_size("ctx")
    slots = size * PIECE // (2 * BLOCK)
    device = lax.axis_index("ctx")
    own = jnp.stack((key_states, value_states)).reshape(2, per_dev, BLOCK, kv_heads, head_dim)
    own = jnp.transpose(own, (3, 1, 0, 2, 4)).reshape(kv_heads, per_dev, 2 * BLOCK, head_dim)
    far = shifted(own, "ctx", 2)
    core_kv = to_partner(own, "ctx", 0)
    chip_kv = to_partner(far, "ctx", 1)
    tables = vertical_tables(vert_blocks, vert_count, per_dev, size, slots)
    vert = spread_vertical(
        own.reshape(kv_heads * per_dev, 2 * BLOCK, head_dim), tables, device, "ctx"
    )
    rank = tables[1]
    spots = jnp.stack((rank % slots, rank // slots), axis=1).reshape(-1)
    lists = tile_lists(vert_blocks, vert_count, slash_offsets, slash_count, device, per_dev)
    queries = jnp.moveaxis(query_states.reshape(rows_dev, kv_heads, group_size, head_dim), 0, 2)
    core = (device % 2).reshape(1)
    out = attend(queries, own, core_kv, chip_kv, far, vert, lists, spots, core)
    return jnp.transpose(out, (2, 0, 1, 3)).reshape(rows_dev, q_heads, head_dim)


def solution(mesh):
    in_specs = (
        P(("groups", "ctx"), None, None),
        P(("groups", "ctx"), None, None),
        P(("groups", "ctx"), None, None),
        P("groups", None),
        P("groups"),
        P("groups", None),
        P("groups"),
    )
    out_specs = P(("groups", "ctx"), None, None)
    return jax.shard_map(local, mesh=mesh, in_specs=in_specs, out_specs=out_specs, check_vma=False)
```

```python
import functools
import math

import jax
import jax.numpy as jnp
from jax import lax
from jax.experimental import pallas as pl
from jax.experimental.pallas import tpu as pltpu
from jax.sharding import Mesh, PartitionSpec as P

BLOCK = 128
SLOTS = 6
CORES = 2
PAIR = 2
ALL = ("y", "x", "core")


def shifted(x, by):
    size = lax.axis_size(ALL)
    pairs = [(i, i + by) for i in range(size) if 0 <= i + by < size]
    return lax.ppermute(x, ALL, pairs)


def whole_spec(x):
    return pl.BlockSpec(x.shape, lambda *_: (0,) * x.ndim)


def small_call(body, scalars, arrays, out_shape, scratch, name):
    return pl.pallas_call(
        body,
        grid_spec=pltpu.PrefetchScalarGridSpec(
            num_scalar_prefetch=len(scalars),
            grid=(1,),
            in_specs=[whole_spec(a) for a in arrays],
            out_specs=pl.BlockSpec(out_shape, lambda *_: (0,) * len(out_shape)),
            scratch_shapes=scratch,
        ),
        out_shape=jax.ShapeDtypeStruct(out_shape, arrays[0].dtype),
        name=name,
    )(*scalars, *arrays)


def each_tile(verts, counts, per_dev, n_vert, columns):
    for i in range(verts.shape[0]):
        block = verts[i]
        owner = block // per_dev
        used = (i % n_vert) < counts[i // n_vert]
        yield i, used, owner // columns, owner % columns, (i // n_vert) * per_dev + block % per_dev


def pick_body(verts, counts, place, pool, send, *, per_dev, n_vert, columns):
    seen = jnp.int32(0) - place[2] * SLOTS
    for _, used, row, col, tile in each_tile(verts, counts, per_dev, n_vert, columns):
        here = used & (col == place[1])

        @pl.when(here & (row == place[0]) & (seen >= 0) & (seen < SLOTS))
        def _():
            send[:, seen] = pool[tile]

        seen = seen + here.astype(jnp.int32)


def keep_body(verts, counts, place, got, send, *, per_dev, n_vert, columns):
    seen = jnp.int32(0) - place[2] * SLOTS
    for _, used, row, col, _ in each_tile(verts, counts, per_dev, n_vert, columns):
        here = used & (col == place[1])

        @pl.when(here & (seen >= 0) & (seen < SLOTS))
        def _():
            piece = got[row, seen]
            for i in range(send.shape[0]):
                send[i, seen] = piece

        seen = seen + here.astype(jnp.int32)


def merge_body(verts, counts, place, same, other, old, out, seen, *, per_dev, n_vert, columns):
    half = out.shape[0]
    core = place[1] % CORES
    out[...] = old[...]
    for i in range(columns):
        seen[i] = -place[2] * SLOTS
    for i, used, _, col, _ in each_tile(verts, counts, per_dev, n_vert, columns):
        slot = seen[col]
        seen[col] = slot + used.astype(jnp.int32)
        wanted = used & (slot >= 0) & (slot < SLOTS) & (core == i // half)

        @pl.when(wanted & (col % CORES == core))
        def _():
            out[i % half] = same[col // CORES, slot]

        @pl.when(wanted & (col % CORES != core))
        def _():
            out[i % half] = other[col // CORES, slot]


def spread_vertical(pool, verts, counts, device, per_dev, n_vert):
    rows_y, cols_x = lax.axis_size("y"), lax.axis_size("x")
    columns = cols_x * CORES
    n_tiles, tile_rows, width = pool.shape
    piece = tile_rows // rows_y
    half = len(verts) // CORES
    static = dict(per_dev=per_dev, n_vert=n_vert, columns=columns)
    pool = pool.reshape(n_tiles, rows_y, piece, width)
    swap = lambda x: lax.ppermute(x, "core", [(0, 1), (1, 0)])

    def turn(t, kept):
        place = jnp.stack((device // columns, device % columns, t)).astype(jnp.int32)
        scalars = (verts, counts, place)
        shape_y = (rows_y, SLOTS, piece, width)
        shape_x = (cols_x, SLOTS, piece, width)
        send = small_call(
            functools.partial(pick_body, **static), scalars, (pool,), shape_y, [], "pick"
        )
        got = lax.all_to_all(send, "y", 0, 0, tiled=True)
        send = small_call(
            functools.partial(keep_body, **static), scalars, (got,), shape_x, [], "keep"
        )
        same = lax.all_to_all(send, "x", 0, 0, tiled=True)
        return small_call(
            functools.partial(merge_body, **static), scalars, (same, swap(same), kept),
            kept.shape, [pltpu.SMEM((columns,), jnp.int32)], "merge",
        )

    used = (jnp.arange(n_vert)[None, :] < counts[:, None]).reshape(-1)
    column_of = (verts // per_dev) % columns
    load = jnp.sum((column_of[None, :] == jnp.arange(columns)[:, None]) & used, axis=1)
    turns = (jnp.max(load) + SLOTS - 1) // SLOTS
    first = turn(jnp.int32(0), jnp.zeros((half, piece, width), pool.dtype))
    held = lax.while_loop(
        lambda c: c[0] < turns, lambda c: (c[0] + 1, turn(c[0], c[1])), (jnp.int32(1), first)
    )[1]
    mine = lax.all_to_all(
        jnp.broadcast_to(held, (rows_y, *held.shape)), "y", 0, 0, tiled=True
    )
    return mine, swap(mine)


def attend_body(
    verts, vert_count, slashes, slash_count, place, q_ref, own_ref, core_ref, chip_ref, far_ref,
    mine_ref, theirs_ref, out_ref, keys, vals, wide, lists, *, n_vert, n_slash, per_dev, half,
):
    step = pl.program_id(0)
    group, _, dim = q_ref.shape[1:]
    scale = math.log2(math.e) / math.sqrt(dim)
    core = place[0] % CORES
    window = 3 * per_dev
    most = n_vert + n_slash

    @pl.when(step == 0)
    def _():
        vals[:, :, :, dim:] = jnp.ones((*vals.shape[:3], dim), vals.dtype)

    for hh in range(PAIR):
        def put(at, tile):
            keys[hh, at] = tile[:BLOCK]
            vals[hh, at, :, :dim] = tile[BLOCK:]

        for i in range(per_dev):
            put(i, far_ref[hh, i])
            put(2 * per_dev + i, own_ref[hh, i])

        @pl.when(core == 1)
        def _():
            for i in range(per_dev):
                put(per_dev + i, core_ref[hh, i])

        @pl.when(core == 0)
        def _():
            for i in range(per_dev):
                put(per_dev + i, chip_ref[hh, i])

        first = (step * PAIR + hh) * n_vert

        @pl.when(first // half == core)
        def _():
            for i in range(n_vert):
                put(window + i, mine_ref[:, first % half + i].reshape(2 * BLOCK, dim))

        @pl.when(first // half != core)
        def _():
            for i in range(n_vert):
                put(window + i, theirs_ref[:, first % half + i].reshape(2 * BLOCK, dim))

    row = lax.broadcasted_iota(jnp.int32, (BLOCK, BLOCK), 0)
    col = lax.broadcasted_iota(jnp.int32, (BLOCK, BLOCK), 1)
    causal = jnp.concatenate([col <= row] * 2, axis=0)

    def block(l, carry):
        qblock = place[0] * per_dev + l
        for hh in range(PAIR):
            head = step * PAIR + hh
            n_used = vert_count[head]
            count = jnp.int32(1)
            for i in range(n_slash):
                offset = slashes[head * n_slash + i]
                block_at = qblock - offset
                ok = (i < slash_count[head]) & (offset > 0) & (block_at >= 0)
                for j in range(n_vert):
                    ok = ok & jnp.logical_not((j < n_used) & (verts[head * n_vert + j] == block_at))
                lists[count] = l - offset + 2 * per_dev
                count = count + ok.astype(jnp.int32)
            for j in range(n_vert):
                ok = (j < n_used) & (verts[head * n_vert + j] < qblock)
                lists[count] = jnp.int32(window + j)
                count = count + ok.astype(jnp.int32)

            def run(n):
                at = [2 * per_dev + l] + [lists[i] for i in range(1, n)]
                k = jnp.concatenate([keys[hh, i] for i in at], axis=0)
                v = jnp.concatenate([vals[hh, i] for i in at], axis=0)
                for r in range(0, group, 2):
                    q = q_ref[hh, r : r + 2, pl.ds(l * BLOCK, BLOCK), :].reshape(2 * BLOCK, dim)
                    s = lax.dot_general(
                        q, k, (((1,), (1,)), ((), ())), preferred_element_type=jnp.float32
                    )
                    parts = [s[:, i * BLOCK : (i + 1) * BLOCK] for i in range(n)]
                    parts[0] = jnp.where(causal, parts[0], -jnp.inf)
                    top = functools.reduce(jnp.maximum, parts)
                    top = jnp.max(top, axis=-1, keepdims=True) * scale
                    p = jnp.concatenate(
                        [jnp.exp2(x * scale - top).astype(jnp.bfloat16) for x in parts], axis=1
                    )
                    o = jnp.dot(p, v, preferred_element_type=jnp.float32)
                    o = o[:, :dim] / o[:, dim:]
                    for i in range(2):
                        wide[pl.ds(hh * group + r + i, BLOCK, stride=PAIR * group), :] = o[
                            i * BLOCK : (i + 1) * BLOCK
                        ]

            for n in range(1, most + 1):
                pl.when(count == n)(functools.partial(run, n))
        out_ref[pl.ds(l * BLOCK, BLOCK)] = (
            wide[...].reshape(BLOCK, PAIR * group, dim).astype(out_ref.dtype)
        )
        return carry

    lax.fori_loop(0, per_dev, block, 0)


def attend(
    queries, own, core_kv, chip_kv, far, mine, theirs, verts, vert_count, slashes, slash_count,
    device,
):
    heads, group, rows, dim = queries.shape
    per_dev = own.shape[1]
    n_vert = len(verts) // heads
    n_slash = len(slashes) // heads
    pool = 3 * per_dev + n_vert
    kv_spec = pl.BlockSpec((PAIR, *own.shape[1:]), lambda h, *_: (h, 0, 0, 0))
    return pl.pallas_call(
        functools.partial(
            attend_body, n_vert=n_vert, n_slash=n_slash, per_dev=per_dev, half=mine.shape[1]
        ),
        grid_spec=pltpu.PrefetchScalarGridSpec(
            num_scalar_prefetch=5,
            grid=(heads // PAIR,),
            in_specs=[
                pl.BlockSpec((PAIR, group, rows, dim), lambda h, *_: (h, 0, 0, 0)),
                kv_spec, kv_spec, kv_spec, kv_spec, whole_spec(mine), whole_spec(theirs),
            ],
            out_specs=pl.BlockSpec((rows, PAIR * group, dim), lambda h, *_: (0, h, 0)),
            scratch_shapes=[
                pltpu.VMEM((PAIR, pool, BLOCK, dim), own.dtype),
                pltpu.VMEM((PAIR, pool, BLOCK, 2 * dim), own.dtype),
                pltpu.VMEM((BLOCK * PAIR * group, dim), jnp.float32),
                pltpu.SMEM((n_vert + n_slash + 1,), jnp.int32),
            ],
        ),
        out_shape=jax.ShapeDtypeStruct((rows, heads * group, dim), queries.dtype),
        name="attend",
    )(
        verts, vert_count, slashes, slash_count, device.reshape(1),
        queries, own, core_kv, chip_kv, far, mine, theirs,
    )


def local(
    query_states, key_states, value_states, vert_blocks, vert_count, slash_offsets, slash_count
):
    rows_dev, q_heads, head_dim = query_states.shape
    kv_heads = key_states.shape[1]
    group_size = q_heads // kv_heads
    per_dev = rows_dev // BLOCK
    n_vert = vert_blocks.shape[1]
    device = lax.axis_index(ALL).astype(jnp.int32)
    own = jnp.stack((key_states, value_states)).reshape(2, per_dev, BLOCK, kv_heads, head_dim)
    own = jnp.transpose(own, (3, 1, 0, 2, 4)).reshape(kv_heads, per_dev, 2 * BLOCK, head_dim)
    far = shifted(own, 2)
    core_kv = lax.ppermute(own, "core", [(0, 1)])
    chip_kv = lax.ppermute(far, "core", [(1, 0)])
    verts = vert_blocks.reshape(-1)
    mine, theirs = spread_vertical(
        own.reshape(kv_heads * per_dev, 2 * BLOCK, head_dim),
        verts, vert_count, device, per_dev, n_vert,
    )
    queries = jnp.moveaxis(query_states.reshape(rows_dev, kv_heads, group_size, head_dim), 0, 2)
    return attend(
        queries, own, core_kv, chip_kv, far, mine, theirs,
        verts, vert_count, slash_offsets.reshape(-1), slash_count, device,
    )


def solution(mesh):
    groups, size = mesh.shape["groups"], mesh.shape["ctx"]
    side = math.isqrt(size // CORES)
    parts = Mesh(
        mesh.devices.reshape(groups, size // (CORES * side), side, CORES), ("groups", *ALL)
    )
    rows = P(("groups", *ALL), None, None)
    in_specs = (rows, rows, rows, P("groups", None), P("groups"), P("groups", None), P("groups"))
    return jax.shard_map(local, mesh=parts, in_specs=in_specs, out_specs=rows, check_vma=False)
```

```python
import functools
import math

import jax
import jax.numpy as jnp
from jax import lax
from jax.experimental import pallas as pl
from jax.experimental.pallas import tpu as pltpu
from jax.sharding import Mesh, PartitionSpec as P


BLOCK = 128
SLOTS = 6
CORES = 2
PAIR = 2
ALL = ("y", "x", "core")


def shifted(x, by):
    size = lax.axis_size(ALL)
    pairs = [(i, i + by) for i in range(size) if 0 <= i + by < size]
    return lax.ppermute(x, ALL, pairs)


def whole_spec(x):
    return pl.BlockSpec(x.shape, lambda *_: (0,) * x.ndim)


def small_call(body, scalars, arrays, out_shape, scratch):
    return pl.pallas_call(
        body,
        grid_spec=pltpu.PrefetchScalarGridSpec(
            num_scalar_prefetch=len(scalars),
            grid=(1,),
            in_specs=[whole_spec(a) for a in arrays],
            out_specs=pl.BlockSpec(out_shape, lambda *_: (0,) * len(out_shape)),
            scratch_shapes=scratch,
        ),
        out_shape=jax.ShapeDtypeStruct(out_shape, arrays[0].dtype),
    )(*scalars, *arrays)


def each_tile(verts, counts, per_dev, n_vert, columns):
    for i in range(verts.shape[0]):
        block = verts[i]
        owner = block // per_dev
        used = (i % n_vert) < counts[i // n_vert]
        yield i, used, owner // columns, owner % columns, (i // n_vert) * per_dev + block % per_dev


def pick_body(verts, counts, place, pool, send, *, per_dev, n_vert, columns):
    seen = jnp.int32(0) - place[2] * SLOTS
    for _, used, row, col, tile in each_tile(verts, counts, per_dev, n_vert, columns):
        here = used & (col == place[1])

        @pl.when(here & (row == place[0]) & (seen >= 0) & (seen < SLOTS))
        def _():
            send[:, seen] = pool[tile]

        seen = seen + here.astype(jnp.int32)


def keep_body(verts, counts, place, got, send, *, per_dev, n_vert, columns):
    seen = jnp.int32(0) - place[2] * SLOTS
    for _, used, row, col, _ in each_tile(verts, counts, per_dev, n_vert, columns):
        here = used & (col == place[1])

        @pl.when(here & (seen >= 0) & (seen < SLOTS))
        def _():
            piece = got[row, seen]
            for i in range(send.shape[0]):
                send[i, seen] = piece

        seen = seen + here.astype(jnp.int32)


def merge_body(verts, counts, place, same, other, old, out, seen, *, per_dev, n_vert, columns):
    half = out.shape[0]
    core = place[1] % CORES
    out[...] = old[...]
    for i in range(columns):
        seen[i] = -place[2] * SLOTS
    for i, used, _, col, _ in each_tile(verts, counts, per_dev, n_vert, columns):
        slot = seen[col]
        seen[col] = slot + used.astype(jnp.int32)
        wanted = used & (slot >= 0) & (slot < SLOTS) & (core == i // half)

        @pl.when(wanted & (col % CORES == core))
        def _():
            out[i % half] = same[col // CORES, slot]

        @pl.when(wanted & (col % CORES != core))
        def _():
            out[i % half] = other[col // CORES, slot]


def spread_vertical(pool, verts, counts, device, per_dev, n_vert, rider):
    rows_y, cols_x = lax.axis_size("y"), lax.axis_size("x")
    columns = cols_x * CORES
    n_tiles, tile_rows, width = pool.shape
    piece = tile_rows // rows_y
    half = len(verts) // CORES
    static = dict(per_dev=per_dev, n_vert=n_vert, columns=columns)
    pool = pool.reshape(n_tiles, rows_y, piece, width)
    swap = lambda x: lax.ppermute(x, "core", [(0, 1), (1, 0)])

    def turn(t, kept, rider):
        place = jnp.stack((device // columns, device % columns, t)).astype(jnp.int32)
        scalars = (verts, counts, place)
        shape_y = (rows_y, SLOTS, piece, width)
        shape_x = (cols_x, SLOTS, piece, width)
        send = small_call(functools.partial(pick_body, **static), scalars, (pool,), shape_y, [])
        got = lax.all_to_all(send, "y", 0, 0, tiled=True)
        got, rider = lax.optimization_barrier((got, rider))
        send = small_call(functools.partial(keep_body, **static), scalars, (got,), shape_x, [])
        same = lax.all_to_all(send, "x", 0, 0, tiled=True)
        merged = small_call(
            functools.partial(merge_body, **static), scalars, (same, swap(same), kept),
            kept.shape, [pltpu.SMEM((columns,), jnp.int32)],
        )
        return merged, rider

    used = (jnp.arange(n_vert)[None, :] < counts[:, None]).reshape(-1)
    column_of = (verts // per_dev) % columns
    load = jnp.sum((column_of[None, :] == jnp.arange(columns)[:, None]) & used, axis=1)
    turns = (jnp.max(load) + SLOTS - 1) // SLOTS
    first, rider = turn(jnp.int32(0), jnp.zeros((half, piece, width), pool.dtype), rider)
    held = lax.while_loop(
        lambda c: c[0] < turns, lambda c: (c[0] + 1, turn(c[0], c[1], ())[0]),
        (jnp.int32(1), first),
    )[1]
    mine = lax.all_to_all(
        jnp.broadcast_to(held, (rows_y, *held.shape)), "y", 0, 0, tiled=True
    )
    return mine, swap(mine), rider


def fill_ones(vals, dim):
    vals[:, :, :, dim:] = jnp.ones((*vals.shape[:3], dim), vals.dtype)


def window_body(
    verts, vert_count, slashes, slash_count, place, q_ref, own_ref, core_ref, chip_ref, far_ref,
    part_ref, stat_ref, keys, vals, lists, *, n_vert, n_slash, per_dev,
):
    step = pl.program_id(0)
    group, _, dim = q_ref.shape[1:]
    scale = math.log2(math.e) / math.sqrt(dim)
    core = place[0] % CORES
    most = n_slash + min(n_vert, per_dev - 1)

    @pl.when(step == 0)
    def _():
        fill_ones(vals, dim)

    for hh in range(PAIR):
        def put(at, tile):
            keys[hh, at] = tile[:BLOCK]
            vals[hh, at, :, :dim] = tile[BLOCK:]

        for i in range(per_dev):
            put(i, far_ref[hh, i])
            put(2 * per_dev + i, own_ref[hh, i])

        @pl.when(core == 1)
        def _():
            for i in range(per_dev):
                put(per_dev + i, core_ref[hh, i])

        @pl.when(core == 0)
        def _():
            for i in range(per_dev):
                put(per_dev + i, chip_ref[hh, i])

    row = lax.broadcasted_iota(jnp.int32, (BLOCK, BLOCK), 0)
    col = lax.broadcasted_iota(jnp.int32, (BLOCK, BLOCK), 1)
    causal = jnp.concatenate([col <= row] * 2, axis=0)
    lane = col // (dim // group)

    def block(l, carry):
        qblock = place[0] * per_dev + l
        for hh in range(PAIR):
            head = step * PAIR + hh
            n_used = vert_count[head]
            count = jnp.int32(1)
            for i in range(n_slash):
                offset = slashes[head * n_slash + i]
                block_at = qblock - offset
                ok = (i < slash_count[head]) & (offset > 0) & (block_at >= 0)
                for j in range(n_vert):
                    ok = ok & jnp.logical_not((j < n_used) & (verts[head * n_vert + j] == block_at))
                lists[count] = l - offset + 2 * per_dev
                count = count + ok.astype(jnp.int32)
            for j in range(n_vert):
                at = verts[head * n_vert + j] - place[0] * per_dev
                ok = (j < n_used) & (at >= 0) & (at < l)
                lists[count] = at + 2 * per_dev
                count = count + ok.astype(jnp.int32)

            def run(n):
                at = [2 * per_dev + l] + [lists[i] for i in range(1, n)]
                k = jnp.concatenate([keys[hh, i] for i in at], axis=0)
                v = jnp.concatenate([vals[hh, i] for i in at], axis=0)
                rows = pl.ds(l * BLOCK, BLOCK)
                stat = None
                for r in range(0, group, 2):
                    q = q_ref[hh, r : r + 2, rows, :].reshape(2 * BLOCK, dim)
                    s = lax.dot_general(
                        q, k, (((1,), (1,)), ((), ())), preferred_element_type=jnp.float32
                    )
                    parts = [s[:, i * BLOCK : (i + 1) * BLOCK] for i in range(n)]
                    parts[0] = jnp.where(causal, parts[0], -jnp.inf)
                    top = functools.reduce(jnp.maximum, parts)
                    top = jnp.max(top, axis=-1, keepdims=True) * scale
                    p = jnp.concatenate(
                        [jnp.exp2(x * scale - top).astype(jnp.bfloat16) for x in parts], axis=1
                    )
                    o = jnp.dot(p, v, preferred_element_type=jnp.float32)
                    part_ref[hh, r : r + 2, rows, :] = (o[:, :dim] / o[:, dim:]).reshape(
                        2, BLOCK, dim
                    )
                    logs = top + jnp.log2(o[:, dim:])
                    for i in range(2):
                        mine = logs[i * BLOCK : (i + 1) * BLOCK]
                        stat = mine if stat is None else jnp.where(lane == r + i, mine, stat)
                stat_ref[hh, rows, :] = stat

            for n in range(1, most + 1):
                pl.when(count == n)(functools.partial(run, n))
        return carry

    lax.fori_loop(0, per_dev, block, 0)


def vertical_body(
    verts, vert_count, place, q_ref, part_ref, stat_ref, mine_ref, theirs_ref, out_ref,
    keys, vals, wide, s0, s1, p0, p1, t0, t1, *, n_vert, per_dev, half, chunk,
):
    step = pl.program_id(0)
    group, rows, dim = q_ref.shape[1:]
    scale = math.log2(math.e) / math.sqrt(dim)
    core = place[0] % CORES
    chunks = rows // chunk
    heads = PAIR * group

    @pl.when(step == 0)
    def _():
        fill_ones(vals, dim)

    for hh in range(PAIR):
        first = (step * PAIR + hh) * n_vert

        def take(source):
            count = jnp.int32(0)
            for j in range(n_vert):
                ok = (j < vert_count[step * PAIR + hh]) & (
                    verts[first + j] < place[0] * per_dev
                )

                @pl.when(ok)
                def _():
                    tile = source[:, first % half + j].reshape(2 * BLOCK, dim)
                    keys[hh, count] = tile[:BLOCK]
                    vals[hh, count, :, :dim] = tile[BLOCK:]

                count = count + ok.astype(jnp.int32)

        pl.when(first // half == core)(lambda: take(mine_ref))
        pl.when(first // half != core)(lambda: take(theirs_ref))
        count = jnp.int32(0)
        for j in range(n_vert):
            ok = (j < vert_count[step * PAIR + hh]) & (verts[first + j] < place[0] * per_dev)
            count = count + ok.astype(jnp.int32)

        def store(i, r, value):
            wide[pl.ds(i * chunk * heads + hh * group + r, chunk, stride=heads), :] = value

        def run(n):
            wide_keys = n * BLOCK

            def stages(i, s_in, s_out, p_in, p_out, t_in, t_out):
                at = jnp.minimum(i, chunks - 1)
                q = q_ref[hh, :, pl.ds(at * chunk, chunk), :].reshape(group * chunk, dim)
                k = keys[hh, :n].reshape(wide_keys, dim)
                s_in[:, :wide_keys] = lax.dot_general(
                    q, k, (((1,), (1,)), ((), ())), preferred_element_type=jnp.float32
                ) * scale
                parts = [s_out[:, j * BLOCK : (j + 1) * BLOCK] for j in range(n)]
                top = jnp.max(functools.reduce(jnp.maximum, parts), axis=-1, keepdims=True)
                for j in range(n):
                    p_in[:, j * BLOCK : (j + 1) * BLOCK] = jnp.exp2(parts[j] - top).astype(
                        jnp.bfloat16
                    )
                t_in[...] = jnp.broadcast_to(top, t_in.shape)
                at = jnp.clip(i - 2, 0, chunks - 1)
                v = vals[hh, :n].reshape(wide_keys, 2 * dim)
                o = jnp.dot(p_out[:, :wide_keys], v, preferred_element_type=jnp.float32)
                stat = stat_ref[hh, pl.ds(at * chunk, chunk), :]
                for r in range(group):
                    some = slice(r * chunk, (r + 1) * chunk)
                    lane = r * (dim // group)
                    logs = jnp.broadcast_to(stat[:, lane : lane + 1], (chunk, dim))
                    new = t_out[some]
                    most = jnp.maximum(logs, new)
                    before, after = jnp.exp2(logs - most), jnp.exp2(new - most)
                    whole = part_ref[hh, r, pl.ds(at * chunk, chunk), :] * before
                    whole = whole + o[some, :dim] * after
                    store(at, r, whole / (before + o[some, dim:] * after))

            def two(i, carry):
                stages(2 * i, s0, s1, p1, p0, t1, t0)
                stages(2 * i + 1, s1, s0, p0, p1, t0, t1)
                return carry

            lax.fori_loop(0, (chunks + 2) // 2, two, 0)

        @pl.when(count == 0)
        def _():
            def copy(i, carry):
                for r in range(group):
                    store(i, r, part_ref[hh, r, pl.ds(i * chunk, chunk), :])
                return carry

            lax.fori_loop(0, chunks, copy, 0)

        for n in range(1, n_vert + 1):
            pl.when(count == n)(functools.partial(run, n))

    def write(i, carry):
        some = wide[pl.ds(i * chunk * heads, chunk * heads), :]
        out_ref[pl.ds(i * chunk, chunk)] = some.reshape(chunk, heads, dim).astype(out_ref.dtype)
        return carry

    lax.fori_loop(0, chunks, write, 0)


def cost(queries, tiles):
    size = math.prod(queries.shape)
    return pl.CostEstimate(
        flops=4 * size * BLOCK * tiles, transcendentals=size * tiles, bytes_accessed=8 * size
    )


def attend_window(queries, own, core_kv, chip_kv, far, verts, vert_count, slashes, slash_count, device):
    heads, group, rows, dim = queries.shape
    per_dev = own.shape[1]
    n_vert = len(verts) // heads
    n_slash = len(slashes) // heads
    kv_spec = pl.BlockSpec((PAIR, *own.shape[1:]), lambda h, *_: (h, 0, 0, 0))
    q_spec = pl.BlockSpec((PAIR, group, rows, dim), lambda h, *_: (h, 0, 0, 0))
    return pl.pallas_call(
        functools.partial(window_body, n_vert=n_vert, n_slash=n_slash, per_dev=per_dev),
        grid_spec=pltpu.PrefetchScalarGridSpec(
            num_scalar_prefetch=5,
            grid=(heads // PAIR,),
            in_specs=[q_spec, kv_spec, kv_spec, kv_spec, kv_spec],
            out_specs=[q_spec, pl.BlockSpec((PAIR, rows, dim), lambda h, *_: (h, 0, 0))],
            scratch_shapes=[
                pltpu.VMEM((PAIR, 3 * per_dev, BLOCK, dim), own.dtype),
                pltpu.VMEM((PAIR, 3 * per_dev, BLOCK, 2 * dim), own.dtype),
                pltpu.SMEM((n_vert + n_slash + 1,), jnp.int32),
            ],
        ),
        out_shape=[
            jax.ShapeDtypeStruct(queries.shape, jnp.float32),
            jax.ShapeDtypeStruct((heads, rows, dim), jnp.float32),
        ],
        cost_estimate=cost(queries, n_slash),
        name="window",
    )(
        verts, vert_count, slashes, slash_count, device.reshape(1),
        queries, own, core_kv, chip_kv, far,
    )


def attend_vertical(queries, part, stat, mine, theirs, verts, vert_count, device, per_dev):
    heads, group, rows, dim = queries.shape
    n_vert = len(verts) // heads
    chunk = rows // 8
    lines = group * chunk
    q_spec = pl.BlockSpec((PAIR, group, rows, dim), lambda h, *_: (h, 0, 0, 0))
    scores = pltpu.VMEM((lines, n_vert * BLOCK), jnp.float32)
    powers = pltpu.VMEM((lines, n_vert * BLOCK), queries.dtype)
    tops = pltpu.VMEM((lines, dim), jnp.float32)
    return pl.pallas_call(
        functools.partial(
            vertical_body, n_vert=n_vert, per_dev=per_dev, half=mine.shape[1], chunk=chunk
        ),
        grid_spec=pltpu.PrefetchScalarGridSpec(
            num_scalar_prefetch=3,
            grid=(heads // PAIR,),
            in_specs=[
                q_spec, q_spec, pl.BlockSpec((PAIR, rows, dim), lambda h, *_: (h, 0, 0)),
                whole_spec(mine), whole_spec(theirs),
            ],
            out_specs=pl.BlockSpec((rows, PAIR * group, dim), lambda h, *_: (0, h, 0)),
            scratch_shapes=[
                pltpu.VMEM((PAIR, n_vert, BLOCK, dim), queries.dtype),
                pltpu.VMEM((PAIR, n_vert, BLOCK, 2 * dim), queries.dtype),
                pltpu.VMEM((rows * PAIR * group, dim), jnp.float32),
                scores, scores, powers, powers, tops, tops,
            ],
        ),
        out_shape=jax.ShapeDtypeStruct((rows, heads * group, dim), queries.dtype),
        cost_estimate=cost(queries, n_vert),
        name="vertical",
    )(verts, vert_count, device.reshape(1), queries, part, stat, mine, theirs)


def local(
    query_states, key_states, value_states, vert_blocks, vert_count, slash_offsets, slash_count
):
    rows_dev, q_heads, head_dim = query_states.shape
    kv_heads = key_states.shape[1]
    group_size = q_heads // kv_heads
    per_dev = rows_dev // BLOCK
    n_vert = vert_blocks.shape[1]
    device = lax.axis_index(ALL).astype(jnp.int32)
    own = jnp.stack((key_states, value_states)).reshape(2, per_dev, BLOCK, kv_heads, head_dim)
    own = jnp.transpose(own, (3, 1, 0, 2, 4)).reshape(kv_heads, per_dev, 2 * BLOCK, head_dim)
    far = shifted(own, 2)
    core_kv = lax.ppermute(own, "core", [(0, 1)])
    chip_kv = lax.ppermute(far, "core", [(1, 0)])
    verts = vert_blocks.reshape(-1)
    queries = jnp.moveaxis(query_states.reshape(rows_dev, kv_heads, group_size, head_dim), 0, 2)
    mine, theirs, queries = spread_vertical(
        own.reshape(kv_heads * per_dev, 2 * BLOCK, head_dim),
        verts, vert_count, device, per_dev, n_vert, queries,
    )
    part, stat = attend_window(
        queries, own, core_kv, chip_kv, far,
        verts, vert_count, slash_offsets.reshape(-1), slash_count, device,
    )
    return attend_vertical(
        queries, part, stat, mine, theirs, verts, vert_count, device, per_dev
    )


def solution(mesh):
    groups, size = mesh.shape["groups"], mesh.shape["ctx"]
    side = math.isqrt(size // CORES)
    parts = Mesh(
        mesh.devices.reshape(groups, size // (CORES * side), side, CORES), ("groups", *ALL)
    )
    rows = P(("groups", *ALL), None, None)
    in_specs = (rows, rows, rows, P("groups", None), P("groups"), P("groups", None), P("groups"))
    return jax.shard_map(local, mesh=parts, in_specs=in_specs, out_specs=rows, check_vma=False)
```

```python
import functools
import math

import jax
import jax.numpy as jnp
from jax import lax
from jax.experimental import pallas as pl
from jax.experimental.pallas import tpu as pltpu
from jax.sharding import Mesh, PartitionSpec as P


BLOCK = 128
SLOTS = 6
CORES = 2
PAIR = 2
ALL = ("y", "x", "core")


def hop(x, axis, wrap=False, only=None):
    size = lax.axis_size(axis)
    pairs = [(i, (i + 1) % size) for i in range(size) if wrap or i + 1 < size]
    axes = axis
    if only is not None:
        _, index = only
        axes = ("y", "x")
        width = lax.axis_size("x")
        flat = (lambda i: i * width + index) if axis == "y" else (lambda i: index * width + i)
        pairs = [(flat(i), flat(j)) for i, j in pairs]
    return lax.ppermute(x, axes, pairs)


def from_last_chip(x):
    return lax.ppermute(x, "x", [(lax.axis_size("x") - 1, 0)])


def whole_spec(x):
    return pl.BlockSpec(x.shape, lambda *_: (0,) * x.ndim)


def small_call(body, scalars, arrays, out_shape, scratch):
    return pl.pallas_call(
        body,
        grid_spec=pltpu.PrefetchScalarGridSpec(
            num_scalar_prefetch=len(scalars),
            grid=(1,),
            in_specs=[whole_spec(a) for a in arrays],
            out_specs=pl.BlockSpec(out_shape, lambda *_: (0,) * len(out_shape)),
            scratch_shapes=scratch,
        ),
        out_shape=jax.ShapeDtypeStruct(out_shape, arrays[0].dtype),
    )(*scalars, *arrays)


def each_tile(verts, counts, per_dev, n_vert, columns):
    for i in range(verts.shape[0]):
        block = verts[i]
        owner = block // per_dev
        used = (i % n_vert) < counts[i // n_vert]
        yield i, used, owner // columns, owner % columns, (i // n_vert) * per_dev + block % per_dev


def pick_body(verts, counts, place, pool, send, *, per_dev, n_vert, columns):
    seen = jnp.int32(0) - place[2] * SLOTS
    for _, used, row, col, tile in each_tile(verts, counts, per_dev, n_vert, columns):
        here = used & (col == place[1])

        @pl.when(here & (row == place[0]) & (seen >= 0) & (seen < SLOTS))
        def _():
            send[:, seen] = pool[tile]

        seen = seen + here.astype(jnp.int32)


def keep_body(verts, counts, place, got, send, *, per_dev, n_vert, columns):
    seen = jnp.int32(0) - place[2] * SLOTS
    for _, used, row, col, _ in each_tile(verts, counts, per_dev, n_vert, columns):
        here = used & (col == place[1])

        @pl.when(here & (seen >= 0) & (seen < SLOTS))
        def _():
            piece = got[row, seen]
            for i in range(send.shape[0]):
                send[i, seen] = piece

        seen = seen + here.astype(jnp.int32)


def merge_body(verts, counts, place, same, other, old, out, seen, *, per_dev, n_vert, columns):
    half = out.shape[0]
    core = place[1] % CORES
    out[...] = old[...]
    for i in range(columns):
        seen[i] = -place[2] * SLOTS
    for i, used, _, col, _ in each_tile(verts, counts, per_dev, n_vert, columns):
        slot = seen[col]
        seen[col] = slot + used.astype(jnp.int32)
        wanted = used & (slot >= 0) & (slot < SLOTS) & (core == i // half)

        @pl.when(wanted & (col % CORES == core))
        def _():
            out[i % half] = same[col // CORES, slot]

        @pl.when(wanted & (col % CORES != core))
        def _():
            out[i % half] = other[col // CORES, slot]


def spread_vertical(pool, verts, counts, device, per_dev, n_vert, rider):
    rows_y, cols_x = lax.axis_size("y"), lax.axis_size("x")
    columns = cols_x * CORES
    n_tiles, tile_rows, width = pool.shape
    piece = tile_rows // rows_y
    half = len(verts) // CORES
    static = dict(per_dev=per_dev, n_vert=n_vert, columns=columns)
    pool = pool.reshape(n_tiles, rows_y, piece, width)
    swap = lambda x: lax.ppermute(x, "core", [(0, 1), (1, 0)])

    def turn(t, kept, rider):
        place = jnp.stack((device // columns, device % columns, t)).astype(jnp.int32)
        scalars = (verts, counts, place)
        shape_y = (rows_y, SLOTS, piece, width)
        shape_x = (cols_x, SLOTS, piece, width)
        send = small_call(functools.partial(pick_body, **static), scalars, (pool,), shape_y, [])
        got = lax.all_to_all(send, "y", 0, 0, tiled=True)
        got, rider = lax.optimization_barrier((got, rider))
        send = small_call(functools.partial(keep_body, **static), scalars, (got,), shape_x, [])
        same = lax.all_to_all(send, "x", 0, 0, tiled=True)
        other = swap(same)
        merged = small_call(
            functools.partial(merge_body, **static), scalars, (same, other, kept),
            kept.shape, [pltpu.SMEM((columns,), jnp.int32)],
        )
        return merged, rider

    used = (jnp.arange(n_vert)[None, :] < counts[:, None]).reshape(-1)
    column_of = (verts // per_dev) % columns
    load = jnp.sum((column_of[None, :] == jnp.arange(columns)[:, None]) & used, axis=1)
    turns = (jnp.max(load) + SLOTS - 1) // SLOTS
    first, rider = turn(jnp.int32(0), jnp.zeros((half, piece, width), pool.dtype), rider)
    held = lax.while_loop(
        lambda c: c[0] < turns, lambda c: (c[0] + 1, turn(c[0], c[1], ())[0]),
        (jnp.int32(1), first),
    )[1]
    mine = lax.all_to_all(
        jnp.broadcast_to(held, (rows_y, *held.shape)), "y", 0, 0, tiled=True
    )
    return mine, swap(mine), rider


def fill_ones(vals, dim):
    vals[:, :, :, dim:] = jnp.ones((*vals.shape[:3], dim), vals.dtype)


def window_body(
    verts, vert_count, slashes, slash_count, place, q_ref, own_ref, core_ref, chip_ref, far_ref,
    *rest, n_vert, n_slash, per_dev, skip,
):
    part_ref, stat_ref, keys, vals, lists = rest[-5:]
    step = pl.program_id(0) + skip
    group, _, dim = q_ref.shape[1:]
    scale = math.log2(math.e) / math.sqrt(dim)
    core = place[0] % CORES
    most = n_slash + min(n_vert, per_dev - 1)

    @pl.when(step == skip)
    def _():
        fill_ones(vals, dim)

    for hh in range(PAIR):
        def put(at, tile):
            keys[hh, at] = tile[:BLOCK]
            vals[hh, at, :, :dim] = tile[BLOCK:]

        for i in range(per_dev):
            put(i, far_ref[hh, i])
            put(2 * per_dev + i, own_ref[hh, i])

        @pl.when(core == 1)
        def _():
            for i in range(per_dev):
                put(per_dev + i, core_ref[hh, i])

        @pl.when(core == 0)
        def _():
            for i in range(per_dev):
                put(per_dev + i, chip_ref[hh, i])

    row = lax.broadcasted_iota(jnp.int32, (BLOCK, BLOCK), 0)
    col = lax.broadcasted_iota(jnp.int32, (BLOCK, BLOCK), 1)
    causal = jnp.concatenate([col <= row] * 2, axis=0)
    lane = col // (dim // group)

    def block(item, carry):
        l, hh = item // PAIR, item % PAIR
        qblock = place[0] * per_dev + l
        head = step * PAIR + hh
        n_used = vert_count[head]
        count = jnp.int32(1)
        for i in range(n_slash):
            offset = slashes[head * n_slash + i]
            block_at = qblock - offset
            ok = (i < slash_count[head]) & (offset > 0) & (block_at >= 0)
            for j in range(n_vert):
                ok = ok & jnp.logical_not((j < n_used) & (verts[head * n_vert + j] == block_at))
            lists[count] = l - offset + 2 * per_dev
            count = count + ok.astype(jnp.int32)
        for j in range(n_vert):
            at = verts[head * n_vert + j] - place[0] * per_dev
            ok = (j < n_used) & (at >= 0) & (at < l)
            lists[count] = at + 2 * per_dev
            count = count + ok.astype(jnp.int32)

        def run(n):
            at = [2 * per_dev + l] + [lists[i] for i in range(1, n)]
            k = jnp.concatenate([keys[hh, i] for i in at], axis=0)
            v = jnp.concatenate([vals[hh, i] for i in at], axis=0)
            rows = pl.ds(l * BLOCK, BLOCK)
            stat = None
            for r in range(0, group, 2):
                q = q_ref[hh, r : r + 2, rows, :].reshape(2 * BLOCK, dim)
                s = lax.dot_general(
                    q, k, (((1,), (1,)), ((), ())), preferred_element_type=jnp.float32
                )
                parts = [s[:, i * BLOCK : (i + 1) * BLOCK] for i in range(n)]
                parts[0] = jnp.where(causal, parts[0], -jnp.inf)
                top = functools.reduce(jnp.maximum, parts)
                top = jnp.max(top, axis=-1, keepdims=True) * scale
                p = jnp.concatenate(
                    [jnp.exp2(x * scale - top).astype(jnp.bfloat16) for x in parts], axis=1
                )
                o = jnp.dot(p, v, preferred_element_type=jnp.float32)
                part_ref[hh, r : r + 2, rows, :] = (o[:, :dim] / o[:, dim:]).reshape(
                    2, BLOCK, dim
                )
                logs = top + jnp.log2(o[:, dim:])
                for i in range(2):
                    mine = logs[i * BLOCK : (i + 1) * BLOCK]
                    stat = mine if stat is None else jnp.where(lane == r + i, mine, stat)
            stat_ref[hh, rows, :] = stat

        for n in range(1, most + 1):
            pl.when(count == n)(functools.partial(run, n))
        return carry

    lax.fori_loop(0, per_dev * PAIR, block, 0)


def vertical_body(
    verts, vert_count, place, q_ref, part_ref, stat_ref, tiles_ref,
    *rest, n_vert, per_dev, half, chunk,
):
    out_ref, keys, vals, wide, s0, s1, p0, p1, t0, t1 = rest[-10:]
    step = pl.program_id(0) + place[1] * (half // (PAIR * n_vert))
    group, rows, dim = q_ref.shape[1:]
    scale = math.log2(math.e) / math.sqrt(dim)
    chunks = rows // chunk
    heads = PAIR * group

    @pl.when(pl.program_id(0) == 0)
    def _():
        fill_ones(vals, dim)

    def one_head(hh, carry):
        first = (step * PAIR + hh) * n_vert

        count = jnp.int32(0)
        for j in range(n_vert):
            ok = (j < vert_count[step * PAIR + hh]) & (verts[first + j] < place[0] * per_dev)

            @pl.when(ok)
            def _():
                tile = tiles_ref[:, first % half + j].reshape(2 * BLOCK, dim)
                keys[hh, count] = tile[:BLOCK]
                vals[hh, count, :, :dim] = tile[BLOCK:]

            count = count + ok.astype(jnp.int32)

        def store(i, r, value):
            wide[pl.ds(i * chunk * heads + hh * group + r, chunk, stride=heads), :] = value

        def run(n):
            wide_keys = n * BLOCK

            def stages(i, s_in, s_out, p_in, p_out, t_in, t_out):
                at = jnp.minimum(i, chunks - 1)
                q = q_ref[hh, :, pl.ds(at * chunk, chunk), :].reshape(group * chunk, dim)
                k = keys[hh, :n].reshape(wide_keys, dim)
                s_in[:, :wide_keys] = lax.dot_general(
                    q, k, (((1,), (1,)), ((), ())), preferred_element_type=jnp.float32
                ) * scale
                parts = [s_out[:, j * BLOCK : (j + 1) * BLOCK] for j in range(n)]
                top = jnp.max(functools.reduce(jnp.maximum, parts), axis=-1, keepdims=True)
                for j in range(n):
                    p_in[:, j * BLOCK : (j + 1) * BLOCK] = jnp.exp2(parts[j] - top).astype(
                        jnp.bfloat16
                    )
                t_in[...] = jnp.broadcast_to(top, t_in.shape)
                at = jnp.clip(i - 2, 0, chunks - 1)
                v = vals[hh, :n].reshape(wide_keys, 2 * dim)
                o = jnp.dot(p_out[:, :wide_keys], v, preferred_element_type=jnp.float32)
                stat = stat_ref[hh, pl.ds(at * chunk, chunk), :]
                for r in range(group):
                    some = slice(r * chunk, (r + 1) * chunk)
                    lane = r * (dim // group)
                    logs = jnp.broadcast_to(stat[:, lane : lane + 1], (chunk, dim))
                    new = t_out[some]
                    most = jnp.maximum(logs, new)
                    before, after = jnp.exp2(logs - most), jnp.exp2(new - most)
                    whole = part_ref[hh, r, pl.ds(at * chunk, chunk), :] * before
                    whole = whole + o[some, :dim] * after
                    store(at, r, whole / (before + o[some, dim:] * after))

            def two(i, carry):
                stages(2 * i, s0, s1, p1, p0, t1, t0)
                stages(2 * i + 1, s1, s0, p0, p1, t0, t1)
                return carry

            lax.fori_loop(0, (chunks + 2) // 2, two, 0)

        @pl.when(count == 0)
        def _():
            def copy(i, carry):
                for r in range(group):
                    store(i, r, part_ref[hh, r, pl.ds(i * chunk, chunk), :])
                return carry

            lax.fori_loop(0, chunks, copy, 0)

        for n in range(1, n_vert + 1):
            pl.when(count == n)(functools.partial(run, n))
        return carry

    lax.fori_loop(0, PAIR, one_head, 0)

    def write(i, carry):
        some = wide[pl.ds(i * chunk * heads, chunk * heads), :]
        out_ref[pl.ds(i * chunk, chunk)] = some.reshape(chunk, heads, dim).astype(out_ref.dtype)
        return carry

    lax.fori_loop(0, chunks, write, 0)


def cost(queries, tiles):
    size = math.prod(queries.shape)
    return pl.CostEstimate(
        flops=4 * size * BLOCK * tiles, transcendentals=size * tiles, bytes_accessed=8 * size
    )


def attend_window(
    queries, own, core_kv, chip_kv, far, before, verts, vert_count, slashes, slash_count, device,
    skip,
):
    heads, group, rows, dim = queries.shape
    per_dev = own.shape[1]
    n_vert = len(verts) // heads
    n_slash = len(slashes) // heads
    steps = far.shape[0] // PAIR
    shifted = lambda h, *_: (h + skip, 0, 0, 0)
    whole_kv = pl.BlockSpec((PAIR, *own.shape[1:]), shifted)
    half_kv = pl.BlockSpec((PAIR, *own.shape[1:]), lambda h, *_: (h, 0, 0, 0))
    q_spec = pl.BlockSpec((PAIR, group, rows, dim), shifted)
    out_shape = [
        jax.ShapeDtypeStruct(queries.shape, jnp.float32),
        jax.ShapeDtypeStruct((heads, rows, dim), jnp.float32),
    ]
    return pl.pallas_call(
        functools.partial(
            window_body, n_vert=n_vert, n_slash=n_slash, per_dev=per_dev, skip=skip
        ),
        grid_spec=pltpu.PrefetchScalarGridSpec(
            num_scalar_prefetch=5,
            grid=(steps,),
            in_specs=[q_spec, whole_kv, whole_kv, half_kv, half_kv]
            + [pl.BlockSpec(memory_space=pl.ANY)] * len(before),
            out_specs=[q_spec, pl.BlockSpec((PAIR, rows, dim), lambda h, *_: (h + skip, 0, 0))],
            scratch_shapes=[
                pltpu.VMEM((PAIR, 3 * per_dev, BLOCK, dim), own.dtype),
                pltpu.VMEM((PAIR, 3 * per_dev, BLOCK, 2 * dim), own.dtype),
                pltpu.SMEM((n_vert + n_slash + 1,), jnp.int32),
            ],
        ),
        out_shape=out_shape,
        input_output_aliases={10 + i: i for i in range(len(before))},
        cost_estimate=cost(queries, n_slash // 2),
    )(
        verts, vert_count, slashes, slash_count, device.reshape(1),
        queries, own, core_kv, chip_kv, far, *before,
    )


def attend_vertical(queries, part, stat, tiles, before, verts, vert_count, device, which, per_dev):
    heads, group, rows, dim = queries.shape
    n_vert = len(verts) // heads
    chunk = rows // 8
    lines = group * chunk
    half = tiles.shape[1]
    steps = half // (PAIR * n_vert)
    at = lambda h, place: h + place[1] * steps
    q_spec = pl.BlockSpec((PAIR, group, rows, dim), lambda h, v, c, place: (at(h, place), 0, 0, 0))
    scores = pltpu.VMEM((lines, n_vert * BLOCK), jnp.float32)
    powers = pltpu.VMEM((lines, n_vert * BLOCK), queries.dtype)
    tops = pltpu.VMEM((lines, dim), jnp.float32)
    return pl.pallas_call(
        functools.partial(vertical_body, n_vert=n_vert, per_dev=per_dev, half=half, chunk=chunk),
        grid_spec=pltpu.PrefetchScalarGridSpec(
            num_scalar_prefetch=3,
            grid=(steps,),
            in_specs=[
                q_spec, q_spec,
                pl.BlockSpec((PAIR, rows, dim), lambda h, v, c, place: (at(h, place), 0, 0)),
                whole_spec(tiles),
            ]
            + [pl.BlockSpec(memory_space=pl.ANY)] * len(before),
            out_specs=pl.BlockSpec(
                (rows, PAIR * group, dim), lambda h, v, c, place: (0, at(h, place), 0)
            ),
            scratch_shapes=[
                pltpu.VMEM((PAIR, n_vert, BLOCK, dim), queries.dtype),
                pltpu.VMEM((PAIR, n_vert, BLOCK, 2 * dim), queries.dtype),
                pltpu.VMEM((rows * PAIR * group, dim), jnp.float32),
                scores, scores, powers, powers, tops, tops,
            ],
        ),
        out_shape=jax.ShapeDtypeStruct((rows, heads * group, dim), queries.dtype),
        input_output_aliases={7 + i: i for i in range(len(before))},
        cost_estimate=cost(queries, n_vert // 2),
    )(
        verts, vert_count, jnp.stack((device, which)), queries, part, stat, tiles, *before
    )


def local(
    query_states, key_states, value_states, vert_blocks, vert_count, slash_offsets, slash_count
):
    rows_dev, q_heads, head_dim = query_states.shape
    kv_heads = key_states.shape[1]
    group_size = q_heads // kv_heads
    per_dev = rows_dev // BLOCK
    n_vert = vert_blocks.shape[1]
    device = lax.axis_index(ALL).astype(jnp.int32)
    core = device % CORES
    own = jnp.stack((key_states, value_states)).reshape(2, per_dev, BLOCK, kv_heads, head_dim)
    own = jnp.transpose(own, (3, 1, 0, 2, 4)).reshape(kv_heads, per_dev, 2 * BLOCK, head_dim)
    half = kv_heads // 2
    row_end = lax.axis_size("x") - 1
    at_start = lax.axis_index("x") == 0
    low = hop(own[:half], "x", wrap=True)
    low_wrap = hop(low, "y", only=("x", 0))
    high = hop(own[half:], "x")
    high_wrap = hop(own[half:], "y", only=("x", row_end))
    high_wrap = from_last_chip(high_wrap)
    core_kv = lax.ppermute(own, "core", [(0, 1)])
    verts = vert_blocks.reshape(-1)
    slashes = slash_offsets.reshape(-1)
    queries = jnp.moveaxis(query_states.reshape(rows_dev, kv_heads, group_size, head_dim), 0, 2)
    mine, theirs, queries = spread_vertical(
        own.reshape(kv_heads * per_dev, 2 * BLOCK, head_dim),
        verts, vert_count, device, per_dev, n_vert, queries,
    )
    low = jnp.where(at_start, low_wrap, low)
    high = jnp.where(at_start, high_wrap, high)
    low_chip = lax.ppermute(low, "core", [(1, 0)])
    high_chip = lax.ppermute(high, "core", [(1, 0)])
    lists = (verts, vert_count, slashes, slash_count, device)
    state = attend_window(queries, own, core_kv, low_chip, low, (), *lists, 0)
    state = attend_window(queries, own, core_kv, high_chip, high, state, *lists, half // PAIR)
    lists = (verts, vert_count, device)
    out = attend_vertical(queries, *state, mine, (), *lists, core, per_dev)
    return attend_vertical(queries, *state, theirs, (out,), *lists, 1 - core, per_dev)


def solution(mesh):
    groups, size = mesh.shape["groups"], mesh.shape["ctx"]
    side = math.isqrt(size // CORES)
    parts = Mesh(
        mesh.devices.reshape(groups, size // (CORES * side), side, CORES), ("groups", *ALL)
    )
    rows = P(("groups", *ALL), None, None)
    in_specs = (rows, rows, rows, P("groups", None), P("groups"), P("groups", None), P("groups"))
    return jax.shard_map(local, mesh=parts, in_specs=in_specs, out_specs=rows, check_vma=False)
```

```python
import functools
import math

import jax
import jax.numpy as jnp
from jax import lax
from jax.experimental import pallas as pl
from jax.experimental.pallas import tpu as pltpu
from jax.sharding import Mesh, PartitionSpec as P


BLOCK = 128
SLOTS = 6
CORES = 2
PAIR = 2
ALL = ("y", "x", "core")


def hop(x, axis, wrap=False, only=None):
    size = lax.axis_size(axis)
    pairs = [(i, (i + 1) % size) for i in range(size) if wrap or i + 1 < size]
    axes = axis
    if only is not None:
        _, index = only
        axes = ("y", "x")
        width = lax.axis_size("x")
        flat = (lambda i: i * width + index) if axis == "y" else (lambda i: index * width + i)
        pairs = [(flat(i), flat(j)) for i, j in pairs]
    return lax.ppermute(x, axes, pairs)


def from_last_chip(x):
    return lax.ppermute(x, "x", [(lax.axis_size("x") - 1, 0)])


def whole_spec(x):
    return pl.BlockSpec(x.shape, lambda *_: (0,) * x.ndim)


def small_call(body, scalars, arrays, out_shape, scratch):
    return pl.pallas_call(
        body,
        grid_spec=pltpu.PrefetchScalarGridSpec(
            num_scalar_prefetch=len(scalars),
            grid=(1,),
            in_specs=[whole_spec(a) for a in arrays],
            out_specs=pl.BlockSpec(out_shape, lambda *_: (0,) * len(out_shape)),
            scratch_shapes=scratch,
        ),
        out_shape=jax.ShapeDtypeStruct(out_shape, arrays[0].dtype),
    )(*scalars, *arrays)


def each_tile(verts, counts, per_dev, n_vert, columns):
    for i in range(verts.shape[0]):
        block = verts[i]
        owner = block // per_dev
        used = (i % n_vert) < counts[i // n_vert]
        yield i, used, owner // columns, owner % columns, (i // n_vert) * per_dev + block % per_dev


def pick_body(verts, counts, place, low, high, send, *, per_dev, n_vert, columns):
    seen = jnp.int32(0) - place[2] * SLOTS
    for i, used, row, col, tile in each_tile(verts, counts, per_dev, n_vert, columns):
        here = used & (col == place[1])
        first = i // n_vert * per_dev < low.shape[0]
        pool, base = (low, 0) if first else (high, low.shape[0])

        @pl.when(here & (row == place[0]) & (seen >= 0) & (seen < SLOTS))
        def _():
            send[:, seen] = pool[tile - base]

        seen = seen + here.astype(jnp.int32)


def keep_body(verts, counts, place, got, send, *, per_dev, n_vert, columns):
    seen = jnp.int32(0) - place[2] * SLOTS
    for _, used, row, col, _ in each_tile(verts, counts, per_dev, n_vert, columns):
        here = used & (col == place[1])

        @pl.when(here & (seen >= 0) & (seen < SLOTS))
        def _():
            piece = got[row, seen]
            for i in range(send.shape[0]):
                send[i, seen] = piece

        seen = seen + here.astype(jnp.int32)


def merge_body(verts, counts, place, same, other, old, out, seen, *, per_dev, n_vert, columns):
    half = out.shape[0]
    core = place[1] % CORES
    out[...] = old[...]
    for i in range(columns):
        seen[i] = -place[2] * SLOTS
    for i, used, _, col, _ in each_tile(verts, counts, per_dev, n_vert, columns):
        slot = seen[col]
        seen[col] = slot + used.astype(jnp.int32)
        wanted = used & (slot >= 0) & (slot < SLOTS) & (core == i // half)

        @pl.when(wanted & (col % CORES == core))
        def _():
            out[i % half] = same[col // CORES, slot]

        @pl.when(wanted & (col % CORES != core))
        def _():
            out[i % half] = other[col // CORES, slot]


def spread_vertical(low, high, verts, counts, device, per_dev, n_vert, rider):
    rows_y, cols_x = lax.axis_size("y"), lax.axis_size("x")
    columns = cols_x * CORES
    tile_rows, width = low.shape[2:]
    piece = tile_rows // rows_y
    half = len(verts) // CORES
    static = dict(per_dev=per_dev, n_vert=n_vert, columns=columns)
    pools = tuple(x.reshape(-1, rows_y, piece, width) for x in (low, high))
    swap = lambda x: lax.ppermute(x, "core", [(0, 1), (1, 0)])

    def turn(t, kept, rider):
        place = jnp.stack((device // columns, device % columns, t)).astype(jnp.int32)
        scalars = (verts, counts, place)
        shape_y = (rows_y, SLOTS, piece, width)
        shape_x = (cols_x, SLOTS, piece, width)
        send = small_call(functools.partial(pick_body, **static), scalars, pools, shape_y, [])
        got = lax.all_to_all(send, "y", 0, 0, tiled=True)
        got, rider = lax.optimization_barrier((got, rider))
        send = small_call(functools.partial(keep_body, **static), scalars, (got,), shape_x, [])
        same = lax.all_to_all(send, "x", 0, 0, tiled=True)
        other = swap(same)
        merged = small_call(
            functools.partial(merge_body, **static), scalars, (same, other, kept),
            kept.shape, [pltpu.SMEM((columns,), jnp.int32)],
        )
        return merged, rider

    used = (jnp.arange(n_vert)[None, :] < counts[:, None]).reshape(-1)
    column_of = (verts // per_dev) % columns
    load = jnp.sum((column_of[None, :] == jnp.arange(columns)[:, None]) & used, axis=1)
    turns = (jnp.max(load) + SLOTS - 1) // SLOTS
    first, rider = turn(jnp.int32(0), jnp.zeros((half, piece, width), low.dtype), rider)
    held = lax.while_loop(
        lambda c: c[0] < turns, lambda c: (c[0] + 1, turn(c[0], c[1], ())[0]),
        (jnp.int32(1), first),
    )[1]
    mine = lax.all_to_all(
        jnp.broadcast_to(held, (rows_y, *held.shape)), "y", 0, 0, tiled=True
    )
    return mine, swap(mine), rider


def fill_ones(vals, dim):
    vals[..., dim:] = jnp.ones((*vals.shape[:-1], dim), vals.dtype)


def window_body(
    verts, vert_count, slashes, slash_count, place, q_ref, own_ref, core_ref, chip_ref, far_ref,
    part_ref, stat_ref, keys, vals, lists, *, n_vert, n_slash, per_dev, skip,
):
    group, _, dim = q_ref.shape[1:]
    scale = math.log2(math.e) / math.sqrt(dim)
    core = place[0] % CORES
    most = n_slash + min(n_vert, per_dev - 1)

    fill_ones(vals, dim)

    def load(hh, carry):
        def put(at, tile):
            keys[hh, at] = tile[:BLOCK]
            vals[hh, at, :, :dim] = tile[BLOCK:]

        for i in range(per_dev):
            put(i, far_ref[hh, i])
            put(2 * per_dev + i, own_ref[hh, i])

        @pl.when(core == 1)
        def _():
            for i in range(per_dev):
                put(per_dev + i, core_ref[hh, i])

        @pl.when(core == 0)
        def _():
            for i in range(per_dev):
                put(per_dev + i, chip_ref[hh, i])

        return carry

    lax.fori_loop(0, part_ref.shape[0], load, 0)

    row = lax.broadcasted_iota(jnp.int32, (BLOCK, BLOCK), 0)
    col = lax.broadcasted_iota(jnp.int32, (BLOCK, BLOCK), 1)
    causal = jnp.concatenate([col <= row] * 2, axis=0)
    lane = col // (dim // group)

    def block(item, carry):
        hh, l = item // per_dev, item % per_dev
        qblock = place[0] * per_dev + l
        head = skip + hh
        n_used = vert_count[head]
        count = jnp.int32(1)
        for i in range(n_slash):
            offset = slashes[head * n_slash + i]
            block_at = qblock - offset
            ok = (i < slash_count[head]) & (offset > 0) & (block_at >= 0)
            for j in range(n_vert):
                ok = ok & jnp.logical_not((j < n_used) & (verts[head * n_vert + j] == block_at))
            lists[count] = l - offset + 2 * per_dev
            count = count + ok.astype(jnp.int32)
        for j in range(n_vert):
            at = verts[head * n_vert + j] - place[0] * per_dev
            ok = (j < n_used) & (at >= 0) & (at < l)
            lists[count] = at + 2 * per_dev
            count = count + ok.astype(jnp.int32)

        def run(n):
            at = [2 * per_dev + l] + [lists[i] for i in range(1, n)]
            k = jnp.concatenate([keys[hh, i] for i in at], axis=0)
            v = jnp.concatenate([vals[hh, i] for i in at], axis=0)
            rows = pl.ds(l * BLOCK, BLOCK)
            stat = None
            for r in range(0, group, 2):
                q = q_ref[head, r : r + 2, rows, :].reshape(2 * BLOCK, dim)
                s = lax.dot_general(
                    q, k, (((1,), (1,)), ((), ())), preferred_element_type=jnp.float32
                )
                parts = [s[:, i * BLOCK : (i + 1) * BLOCK] for i in range(n)]
                parts[0] = jnp.where(causal, parts[0], -jnp.inf)
                top = functools.reduce(jnp.maximum, parts)
                top = jnp.max(top, axis=-1, keepdims=True) * scale
                p = jnp.concatenate(
                    [jnp.exp2(x * scale - top).astype(jnp.bfloat16) for x in parts], axis=1
                )
                o = jnp.dot(p, v, preferred_element_type=jnp.float32)
                part_ref[hh, r : r + 2, rows, :] = (o[:, :dim] / o[:, dim:]).reshape(
                    2, BLOCK, dim
                )
                logs = top + jnp.log2(o[:, dim:])
                for i in range(2):
                    mine = logs[i * BLOCK : (i + 1) * BLOCK]
                    stat = mine if stat is None else jnp.where(lane == r + i, mine, stat)
            stat_ref[hh, rows, :] = stat

        for n in range(1, most + 1):
            pl.when(count == n)(functools.partial(run, n))
        return carry

    lax.fori_loop(0, per_dev * part_ref.shape[0], block, 0)


def vertical_body(
    verts, vert_count, place, q_ref, low_part, low_stat, high_part, high_stat, tiles_ref,
    *rest, n_vert, per_dev, half, chunk,
):
    out_ref, keys, vals, wide, made, s0, s1, p0, p1, t0, t1, sent = rest[-12:]
    heads_here = half // n_vert
    group, rows, dim = q_ref.shape[1:]
    scale = math.log2(math.e) / math.sqrt(dim)
    chunks = rows // chunk
    heads = PAIR * group

    fill_ones(vals, dim)

    def one_head(at_half, part_ref, stat_ref):
        hh = at_half % PAIR
        head = place[1] * heads_here + at_half
        first = head * n_vert

        count = jnp.int32(0)
        for j in range(n_vert):
            ok = (j < vert_count[head]) & (verts[first + j] < place[0] * per_dev)

            @pl.when(ok)
            def _():
                tile = tiles_ref[:, first % half + j].reshape(2 * BLOCK, dim)
                keys[count] = tile[:BLOCK]
                vals[count, :, :dim] = tile[BLOCK:]

            count = count + ok.astype(jnp.int32)

        def store(i, r, value):
            wide[pl.ds(i * chunk * heads + hh * group + r, chunk, stride=heads), :] = value

        def run(n):
            wide_keys = n * BLOCK

            def stages(i, s_in, s_out, p_in, p_out, t_in, t_out):
                at = jnp.minimum(i, chunks - 1)
                q = q_ref[head, :, pl.ds(at * chunk, chunk), :].reshape(group * chunk, dim)
                k = keys[:n].reshape(wide_keys, dim)
                s_in[:, :wide_keys] = lax.dot_general(
                    q, k, (((1,), (1,)), ((), ())), preferred_element_type=jnp.float32
                ) * scale
                parts = [s_out[:, j * BLOCK : (j + 1) * BLOCK] for j in range(n)]
                top = jnp.max(functools.reduce(jnp.maximum, parts), axis=-1, keepdims=True)
                for j in range(n):
                    p_in[:, j * BLOCK : (j + 1) * BLOCK] = jnp.exp2(parts[j] - top).astype(
                        jnp.bfloat16
                    )
                t_in[...] = jnp.broadcast_to(top, t_in.shape)
                at = jnp.clip(i - 2, 0, chunks - 1)
                v = vals[:n].reshape(wide_keys, 2 * dim)
                o = jnp.dot(p_out[:, :wide_keys], v, preferred_element_type=jnp.float32)
                stat = stat_ref[at_half, pl.ds(at * chunk, chunk), :]
                for r in range(group):
                    some = slice(r * chunk, (r + 1) * chunk)
                    lane = r * (dim // group)
                    logs = jnp.broadcast_to(stat[:, lane : lane + 1], (chunk, dim))
                    new = t_out[some]
                    most = jnp.maximum(logs, new)
                    before, after = jnp.exp2(logs - most), jnp.exp2(new - most)
                    whole = part_ref[at_half, r, pl.ds(at * chunk, chunk), :] * before
                    whole = whole + o[some, :dim] * after
                    store(at, r, whole / (before + o[some, dim:] * after))

            def two(i, carry):
                stages(2 * i, s0, s1, p1, p0, t1, t0)
                stages(2 * i + 1, s1, s0, p0, p1, t0, t1)
                return carry

            lax.fori_loop(0, (chunks + 2) // 2, two, 0)

        @pl.when(count == 0)
        def _():
            def copy(i, carry):
                for r in range(group):
                    store(i, r, part_ref[at_half, r, pl.ds(i * chunk, chunk), :])
                return carry

            lax.fori_loop(0, chunks, copy, 0)

        for n in range(1, n_vert + 1):
            pl.when(count == n)(functools.partial(run, n))

    def pair(i, carry):
        def run_heads(part_ref, stat_ref):
            def step(hh, carry):
                one_head(i * PAIR + hh, part_ref, stat_ref)
                return carry

            lax.fori_loop(0, PAIR, step, 0)

        pl.when(place[1] == 0)(lambda: run_heads(low_part, low_stat))
        pl.when(place[1] == 1)(lambda: run_heads(high_part, high_stat))

        def write(c, carry):
            some = wide[pl.ds(c * chunk * heads, chunk * heads), :]
            made[i, pl.ds(c * chunk, chunk)] = some.reshape(chunk, heads, dim).astype(made.dtype)
            return carry

        lax.fori_loop(0, chunks, write, 0)
        send(i).start()
        return carry

    pairs = heads_here // PAIR

    def send(i):
        at = (place[1] * pairs + i) * heads
        to = out_ref.at[:, pl.ds(pl.multiple_of(at, heads), heads)]
        return pltpu.make_async_copy(made.at[i], to, sent.at[i])

    lax.fori_loop(0, pairs, pair, 0)
    for i in range(pairs):
        send(i).wait()


def cost(queries, tiles):
    size = math.prod(queries.shape)
    return pl.CostEstimate(
        flops=4 * size * BLOCK * tiles, transcendentals=size * tiles, bytes_accessed=8 * size
    )


def in_smem(count):
    return [pl.BlockSpec(memory_space=pltpu.SMEM)] * count


def in_vmem(count):
    return [pl.BlockSpec(memory_space=pltpu.VMEM)] * count


def attend_window(
    queries, own, core_kv, chip_kv, far, verts, vert_count, slashes, slash_count, device, skip
):
    heads, group, rows, dim = queries.shape
    here, per_dev = own.shape[:2]
    n_vert = len(verts) // heads
    n_slash = len(slashes) // heads
    return pl.pallas_call(
        functools.partial(
            window_body, n_vert=n_vert, n_slash=n_slash, per_dev=per_dev, skip=skip
        ),
        in_specs=in_smem(5) + in_vmem(5),
        out_specs=in_vmem(2),
        scratch_shapes=[
            pltpu.VMEM((here, 3 * per_dev, BLOCK, dim), own.dtype),
            pltpu.VMEM((here, 3 * per_dev, BLOCK, 2 * dim), own.dtype),
            pltpu.SMEM((n_vert + n_slash + 1,), jnp.int32),
        ],
        out_shape=[
            jax.ShapeDtypeStruct((here, group, rows, dim), jnp.float32),
            jax.ShapeDtypeStruct((here, rows, dim), jnp.float32),
        ],
        cost_estimate=cost(queries, n_slash // 2),
    )(
        verts, vert_count, slashes, slash_count, device.reshape(1),
        queries, own, core_kv, chip_kv, far,
    )


def attend_vertical(queries, low, high, tiles, before, verts, vert_count, device, which, per_dev):
    heads, group, rows, dim = queries.shape
    n_vert = len(verts) // heads
    chunk = rows // 8
    lines = group * chunk
    half = tiles.shape[1]
    pairs = half // (PAIR * n_vert)
    scores = pltpu.VMEM((lines, n_vert * BLOCK), jnp.float32)
    powers = pltpu.VMEM((lines, n_vert * BLOCK), queries.dtype)
    tops = pltpu.VMEM((lines, dim), jnp.float32)
    return pl.pallas_call(
        functools.partial(vertical_body, n_vert=n_vert, per_dev=per_dev, half=half, chunk=chunk),
        in_specs=in_smem(3) + in_vmem(6) + [pl.BlockSpec(memory_space=pl.ANY)] * len(before),
        out_specs=pl.BlockSpec(memory_space=pl.ANY),
        scratch_shapes=[
            pltpu.VMEM((n_vert, BLOCK, dim), queries.dtype),
            pltpu.VMEM((n_vert, BLOCK, 2 * dim), queries.dtype),
            pltpu.VMEM((rows * PAIR * group, dim), jnp.float32),
            pltpu.VMEM((pairs, rows, PAIR * group, dim), queries.dtype),
            scores, scores, powers, powers, tops, tops,
            pltpu.SemaphoreType.DMA((pairs,)),
        ],
        out_shape=jax.ShapeDtypeStruct((rows, heads * group, dim), queries.dtype),
        input_output_aliases={9 + i: i for i in range(len(before))},
        cost_estimate=cost(queries, n_vert // 2),
    )(
        verts, vert_count, jnp.stack((device, which)), queries, *low, *high, tiles, *before
    )


def local(
    query_states, key_states, value_states, vert_blocks, vert_count, slash_offsets, slash_count
):
    rows_dev, q_heads, head_dim = query_states.shape
    kv_heads = key_states.shape[1]
    group_size = q_heads // kv_heads
    per_dev = rows_dev // BLOCK
    n_vert = vert_blocks.shape[1]
    device = lax.axis_index(ALL).astype(jnp.int32)
    core = device % CORES
    half = kv_heads // 2

    def pool_of(heads):
        both = jnp.stack((key_states[:, heads], value_states[:, heads]))
        both = both.reshape(2, per_dev, BLOCK, half, head_dim)
        return jnp.transpose(both, (3, 1, 0, 2, 4)).reshape(half, per_dev, 2 * BLOCK, head_dim)

    own_low, own_high = pool_of(slice(0, half)), pool_of(slice(half, None))
    row_end = lax.axis_size("x") - 1
    at_start = lax.axis_index("x") == 0
    low = hop(own_low, "x", wrap=True)
    low_wrap = hop(low, "y", only=("x", 0))
    high = hop(own_high, "x")
    high_wrap = hop(own_high, "y", only=("x", row_end))
    high_wrap = from_last_chip(high_wrap)
    core_low = lax.ppermute(own_low, "core", [(0, 1)])
    core_high = lax.ppermute(own_high, "core", [(0, 1)])
    verts = vert_blocks.reshape(-1)
    slashes = slash_offsets.reshape(-1)
    queries = jnp.moveaxis(query_states.reshape(rows_dev, kv_heads, group_size, head_dim), 0, 2)
    mine, theirs, queries = spread_vertical(
        own_low, own_high, verts, vert_count, device, per_dev, n_vert, queries,
    )
    low = jnp.where(at_start, low_wrap, low)
    high = jnp.where(at_start, high_wrap, high)
    low_chip = lax.ppermute(low, "core", [(1, 0)])
    high_chip = lax.ppermute(high, "core", [(1, 0)])
    lists = (verts, vert_count, slashes, slash_count, device)
    low = attend_window(queries, own_low, core_low, low_chip, low, *lists, 0)
    high = attend_window(queries, own_high, core_high, high_chip, high, *lists, half)
    lists = (verts, vert_count, device)
    out = attend_vertical(queries, low, high, mine, (), *lists, core, per_dev)
    return attend_vertical(queries, low, high, theirs, (out,), *lists, 1 - core, per_dev)


def solution(mesh):
    groups, size = mesh.shape["groups"], mesh.shape["ctx"]
    side = math.isqrt(size // CORES)
    parts = Mesh(
        mesh.devices.reshape(groups, size // (CORES * side), side, CORES), ("groups", *ALL)
    )
    rows = P(("groups", *ALL), None, None)
    in_specs = (rows, rows, rows, P("groups", None), P("groups"), P("groups", None), P("groups"))
    return jax.shard_map(local, mesh=parts, in_specs=in_specs, out_specs=rows, check_vma=False)
```

```python
import functools
import math

import jax
import jax.numpy as jnp
from jax import lax
from jax.experimental import pallas as pl
from jax.experimental.pallas import tpu as pltpu
from jax.sharding import Mesh, PartitionSpec as P


BLOCK = 128
SLOTS = 6
CORES = 2
PAIR = 2
WINDOW = 1
ALL = ("y", "x", "core")


def hop(x, axis, wrap=False, only=None):
    size = lax.axis_size(axis)
    pairs = [(i, (i + 1) % size) for i in range(size) if wrap or i + 1 < size]
    axes = axis
    if only is not None:
        _, index = only
        axes = ("y", "x")
        width = lax.axis_size("x")
        flat = (lambda i: i * width + index) if axis == "y" else (lambda i: index * width + i)
        pairs = [(flat(i), flat(j)) for i, j in pairs]
    return lax.ppermute(x, axes, pairs)


def from_last_chip(x):
    return lax.ppermute(x, "x", [(lax.axis_size("x") - 1, 0)])


def whole_spec(x):
    return pl.BlockSpec(x.shape, lambda *_: (0,) * x.ndim)


def small_call(body, scalars, arrays, out_shape, scratch):
    return pl.pallas_call(
        body,
        grid_spec=pltpu.PrefetchScalarGridSpec(
            num_scalar_prefetch=len(scalars),
            grid=(1,),
            in_specs=[whole_spec(a) for a in arrays],
            out_specs=pl.BlockSpec(out_shape, lambda *_: (0,) * len(out_shape)),
            scratch_shapes=scratch,
        ),
        out_shape=jax.ShapeDtypeStruct(out_shape, arrays[0].dtype),
    )(*scalars, *arrays)


def each_tile(verts, counts, per_dev, n_vert, columns):
    for i in range(verts.shape[0]):
        block = verts[i]
        owner = block // per_dev
        used = (i % n_vert) < counts[i // n_vert]
        yield i, used, owner // columns, owner % columns, (i // n_vert) * per_dev + block % per_dev


def pick_body(verts, counts, place, pool, send, *, per_dev, n_vert, columns):
    seen = jnp.int32(0) - place[2] * SLOTS
    for _, used, row, col, tile in each_tile(verts, counts, per_dev, n_vert, columns):
        here = used & (col == place[1])

        @pl.when(here & (row == place[0]) & (seen >= 0) & (seen < SLOTS))
        def _():
            send[:, seen] = pool[tile]

        seen = seen + here.astype(jnp.int32)


def keep_body(verts, counts, place, got, send, *, per_dev, n_vert, columns):
    seen = jnp.int32(0) - place[2] * SLOTS
    for _, used, row, col, _ in each_tile(verts, counts, per_dev, n_vert, columns):
        here = used & (col == place[1])

        @pl.when(here & (seen >= 0) & (seen < SLOTS))
        def _():
            piece = got[row, seen]
            for i in range(send.shape[0]):
                send[i, seen] = piece

        seen = seen + here.astype(jnp.int32)


def merge_body(verts, counts, place, same, other, old, out, seen, *, per_dev, n_vert, columns):
    half = out.shape[0]
    core = place[1] % CORES
    out[...] = old[...]
    for i in range(columns):
        seen[i] = -place[2] * SLOTS
    for i, used, _, col, _ in each_tile(verts, counts, per_dev, n_vert, columns):
        slot = seen[col]
        seen[col] = slot + used.astype(jnp.int32)
        wanted = used & (slot >= 0) & (slot < SLOTS) & (core == i // half)

        @pl.when(wanted & (col % CORES == core))
        def _():
            out[i % half] = same[col // CORES, slot]

        @pl.when(wanted & (col % CORES != core))
        def _():
            out[i % half] = other[col // CORES, slot]


def spread_vertical(pool, verts, counts, device, per_dev, n_vert, rider):
    rows_y, cols_x = lax.axis_size("y"), lax.axis_size("x")
    columns = cols_x * CORES
    n_tiles, tile_rows, width = pool.shape
    piece = tile_rows // rows_y
    half = len(verts) // CORES
    static = dict(per_dev=per_dev, n_vert=n_vert, columns=columns)
    pool = pool.reshape(n_tiles, rows_y, piece, width)
    swap = lambda x: lax.ppermute(x, "core", [(0, 1), (1, 0)])

    def turn(t, kept, rider):
        place = jnp.stack((device // columns, device % columns, t)).astype(jnp.int32)
        scalars = (verts, counts, place)
        shape_y = (rows_y, SLOTS, piece, width)
        shape_x = (cols_x, SLOTS, piece, width)
        send = small_call(functools.partial(pick_body, **static), scalars, (pool,), shape_y, [])
        got = lax.all_to_all(send, "y", 0, 0, tiled=True)
        got, rider = lax.optimization_barrier((got, rider))
        send = small_call(functools.partial(keep_body, **static), scalars, (got,), shape_x, [])
        same = lax.all_to_all(send, "x", 0, 0, tiled=True)
        other = swap(same)
        merged = small_call(
            functools.partial(merge_body, **static), scalars, (same, other, kept),
            kept.shape, [pltpu.SMEM((columns,), jnp.int32)],
        )
        return merged, rider

    used = (jnp.arange(n_vert)[None, :] < counts[:, None]).reshape(-1)
    column_of = (verts // per_dev) % columns
    load = jnp.sum((column_of[None, :] == jnp.arange(columns)[:, None]) & used, axis=1)
    turns = (jnp.max(load) + SLOTS - 1) // SLOTS
    first, rider = turn(jnp.int32(0), jnp.zeros((half, piece, width), pool.dtype), rider)
    held = lax.while_loop(
        lambda c: c[0] < turns, lambda c: (c[0] + 1, turn(c[0], c[1], ())[0]),
        (jnp.int32(1), first),
    )[1]
    mine = lax.all_to_all(
        jnp.broadcast_to(held, (rows_y, *held.shape)), "y", 0, 0, tiled=True
    )
    return mine, swap(mine), rider


def fill_ones(vals, dim):
    vals[..., dim:] = jnp.ones((*vals.shape[:-1], dim), vals.dtype)


def window_body(
    verts, vert_count, slashes, slash_count, place, q_ref, own_ref, core_ref, chip_ref, far_ref,
    *rest, n_vert, n_slash, per_dev, skip,
):
    part_ref, stat_ref, keys, vals, lists = rest[-5:]
    step = pl.program_id(0) + skip
    group, _, dim = q_ref.shape[1:]
    scale = math.log2(math.e) / math.sqrt(dim)
    core = place[0] % CORES
    most = n_slash + min(n_vert, per_dev - 1)

    @pl.when(step == skip)
    def _():
        fill_ones(vals, dim)

    for hh in range(WINDOW):
        def put(at, tile):
            keys[hh, at] = tile[:BLOCK]
            vals[hh, at, :, :dim] = tile[BLOCK:]

        for i in range(per_dev):
            put(i, far_ref[hh, i])
            put(2 * per_dev + i, own_ref[hh, i])

        @pl.when(core == 1)
        def _():
            for i in range(per_dev):
                put(per_dev + i, core_ref[hh, i])

        @pl.when(core == 0)
        def _():
            for i in range(per_dev):
                put(per_dev + i, chip_ref[hh, i])

    row = lax.broadcasted_iota(jnp.int32, (BLOCK, BLOCK), 0)
    col = lax.broadcasted_iota(jnp.int32, (BLOCK, BLOCK), 1)
    causal = jnp.concatenate([col <= row] * 2, axis=0)
    lane = col // (dim // group)

    def block(item, carry):
        l, hh = item // WINDOW, item % WINDOW
        qblock = place[0] * per_dev + l
        head = step * WINDOW + hh
        n_used = vert_count[head]
        count = jnp.int32(1)
        for i in range(n_slash):
            offset = slashes[head * n_slash + i]
            block_at = qblock - offset
            ok = (i < slash_count[head]) & (offset > 0) & (block_at >= 0)
            for j in range(n_vert):
                ok = ok & jnp.logical_not((j < n_used) & (verts[head * n_vert + j] == block_at))
            lists[count] = l - offset + 2 * per_dev
            count = count + ok.astype(jnp.int32)
        for j in range(n_vert):
            at = verts[head * n_vert + j] - place[0] * per_dev
            ok = (j < n_used) & (at >= 0) & (at < l)
            lists[count] = at + 2 * per_dev
            count = count + ok.astype(jnp.int32)

        def run(n):
            at = [2 * per_dev + l] + [lists[i] for i in range(1, n)]
            k = jnp.concatenate([keys[hh, i] for i in at], axis=0)
            v = jnp.concatenate([vals[hh, i] for i in at], axis=0)
            rows = pl.ds(l * BLOCK, BLOCK)
            stat = None
            for r in range(0, group, 2):
                q = q_ref[hh, r : r + 2, rows, :].reshape(2 * BLOCK, dim)
                s = lax.dot_general(
                    q, k, (((1,), (1,)), ((), ())), preferred_element_type=jnp.float32
                )
                parts = [s[:, i * BLOCK : (i + 1) * BLOCK] for i in range(n)]
                parts[0] = jnp.where(causal, parts[0], -jnp.inf)
                top = functools.reduce(jnp.maximum, parts)
                top = jnp.max(top, axis=-1, keepdims=True) * scale
                p = jnp.concatenate(
                    [jnp.exp2(x * scale - top).astype(jnp.bfloat16) for x in parts], axis=1
                )
                o = jnp.dot(p, v, preferred_element_type=jnp.float32)
                part_ref[hh, r : r + 2, rows, :] = (
                    (o[:, :dim] / o[:, dim:]).astype(part_ref.dtype).reshape(2, BLOCK, dim)
                )
                logs = top + jnp.log2(o[:, dim:])
                for i in range(2):
                    mine = logs[i * BLOCK : (i + 1) * BLOCK]
                    stat = mine if stat is None else jnp.where(lane == r + i, mine, stat)
            stat_ref[hh, rows, :] = stat

        for n in range(1, most + 1):
            pl.when(count == n)(functools.partial(run, n))
        return carry

    lax.fori_loop(0, per_dev * WINDOW, block, 0)


def vertical_body(
    verts, vert_count, place, q_ref, part_ref, stat_ref, tiles_ref,
    *rest, n_vert, per_dev, half, chunk,
):
    out_ref, keys, vals, wide, s0, s1, p0, p1, t0, t1 = rest[-10:]
    head = pl.program_id(0) + place[1] * (half // n_vert)
    hh = head % PAIR
    group, rows, dim = q_ref.shape[1:]
    scale = math.log2(math.e) / math.sqrt(dim)
    chunks = rows // chunk
    heads = PAIR * group

    @pl.when(pl.program_id(0) == 0)
    def _():
        fill_ones(vals, dim)

    first = head * n_vert

    count = jnp.int32(0)
    for j in range(n_vert):
        ok = (j < vert_count[head]) & (verts[first + j] < place[0] * per_dev)

        @pl.when(ok)
        def _():
            tile = tiles_ref[:, first % half + j].reshape(2 * BLOCK, dim)
            keys[count] = tile[:BLOCK]
            vals[count, :, :dim] = tile[BLOCK:]

        count = count + ok.astype(jnp.int32)

    def store(i, r, value):
        wide[pl.ds(i * chunk * heads + hh * group + r, chunk, stride=heads), :] = value

    def run(n):
        wide_keys = n * BLOCK

        def stages(i, s_in, s_out, p_in, p_out, t_in, t_out):
            at = jnp.minimum(i, chunks - 1)
            q = q_ref[0, :, pl.ds(at * chunk, chunk), :].reshape(group * chunk, dim)
            k = keys[:n].reshape(wide_keys, dim)
            s_in[:, :wide_keys] = lax.dot_general(
                q, k, (((1,), (1,)), ((), ())), preferred_element_type=jnp.float32
            ) * scale
            parts = [s_out[:, j * BLOCK : (j + 1) * BLOCK] for j in range(n)]
            top = jnp.max(functools.reduce(jnp.maximum, parts), axis=-1, keepdims=True)
            for j in range(n):
                p_in[:, j * BLOCK : (j + 1) * BLOCK] = jnp.exp2(parts[j] - top).astype(
                    jnp.bfloat16
                )
            t_in[...] = jnp.broadcast_to(top, t_in.shape)
            at = jnp.clip(i - 2, 0, chunks - 1)
            v = vals[:n].reshape(wide_keys, 2 * dim)
            o = jnp.dot(p_out[:, :wide_keys], v, preferred_element_type=jnp.float32)
            stat = stat_ref[0, pl.ds(at * chunk, chunk), :]
            for r in range(group):
                some = slice(r * chunk, (r + 1) * chunk)
                lane = r * (dim // group)
                logs = jnp.broadcast_to(stat[:, lane : lane + 1], (chunk, dim))
                new = t_out[some]
                most = jnp.maximum(logs, new)
                before, after = jnp.exp2(logs - most), jnp.exp2(new - most)
                whole = part_ref[0, r, pl.ds(at * chunk, chunk), :].astype(jnp.float32) * before
                whole = whole + o[some, :dim] * after
                store(at, r, whole / (before + o[some, dim:] * after))

        def two(i, carry):
            stages(2 * i, s0, s1, p1, p0, t1, t0)
            stages(2 * i + 1, s1, s0, p0, p1, t0, t1)
            return carry

        lax.fori_loop(0, (chunks + 2) // 2, two, 0)

    @pl.when(count == 0)
    def _():
        def copy(i, carry):
            for r in range(group):
                store(i, r, part_ref[0, r, pl.ds(i * chunk, chunk), :].astype(jnp.float32))
            return carry

        lax.fori_loop(0, chunks, copy, 0)

    for n in range(1, n_vert + 1):
        pl.when(count == n)(functools.partial(run, n))

    def write(i, carry):
        some = wide[pl.ds(i * chunk * heads, chunk * heads), :]
        out_ref[pl.ds(i * chunk, chunk)] = some.reshape(chunk, heads, dim).astype(out_ref.dtype)
        return carry

    @pl.when(hh == PAIR - 1)
    def _():
        lax.fori_loop(0, chunks, write, 0)


def cost(queries, tiles):
    size = math.prod(queries.shape)
    return pl.CostEstimate(
        flops=4 * size * BLOCK * tiles, transcendentals=size * tiles, bytes_accessed=8 * size
    )


def attend_window(
    queries, own, core_kv, chip_kv, far, before, verts, vert_count, slashes, slash_count, device,
    skip,
):
    heads, group, rows, dim = queries.shape
    per_dev = own.shape[1]
    n_vert = len(verts) // heads
    n_slash = len(slashes) // heads
    steps = far.shape[0] // WINDOW
    shifted = lambda h, *_: (h + skip, 0, 0, 0)
    whole_kv = pl.BlockSpec((WINDOW, *own.shape[1:]), shifted)
    half_kv = pl.BlockSpec((WINDOW, *own.shape[1:]), lambda h, *_: (h, 0, 0, 0))
    q_spec = pl.BlockSpec((WINDOW, group, rows, dim), shifted)
    out_shape = [
        jax.ShapeDtypeStruct(queries.shape, queries.dtype),
        jax.ShapeDtypeStruct((heads, rows, dim), jnp.float32),
    ]
    return pl.pallas_call(
        functools.partial(
            window_body, n_vert=n_vert, n_slash=n_slash, per_dev=per_dev, skip=skip
        ),
        grid_spec=pltpu.PrefetchScalarGridSpec(
            num_scalar_prefetch=5,
            grid=(steps,),
            in_specs=[q_spec, whole_kv, whole_kv, half_kv, half_kv]
            + [pl.BlockSpec(memory_space=pl.ANY)] * len(before),
            out_specs=[q_spec, pl.BlockSpec((WINDOW, rows, dim), lambda h, *_: (h + skip, 0, 0))],
            scratch_shapes=[
                pltpu.VMEM((WINDOW, 3 * per_dev, BLOCK, dim), own.dtype),
                pltpu.VMEM((WINDOW, 3 * per_dev, BLOCK, 2 * dim), own.dtype),
                pltpu.SMEM((n_vert + n_slash + 1,), jnp.int32),
            ],
        ),
        out_shape=out_shape,
        input_output_aliases={10 + i: i for i in range(len(before))},
        cost_estimate=cost(queries, n_slash // 2),
    )(
        verts, vert_count, slashes, slash_count, device.reshape(1),
        queries, own, core_kv, chip_kv, far, *before,
    )


def attend_vertical(queries, part, stat, tiles, before, verts, vert_count, device, which, per_dev):
    heads, group, rows, dim = queries.shape
    n_vert = len(verts) // heads
    chunk = rows // 8
    lines = group * chunk
    half = tiles.shape[1]
    steps = half // n_vert
    at = lambda h, place: h + place[1] * steps
    q_spec = pl.BlockSpec((1, group, rows, dim), lambda h, v, c, place: (at(h, place), 0, 0, 0))
    scores = pltpu.VMEM((lines, n_vert * BLOCK), jnp.float32)
    powers = pltpu.VMEM((lines, n_vert * BLOCK), queries.dtype)
    tops = pltpu.VMEM((lines, dim), jnp.float32)
    return pl.pallas_call(
        functools.partial(vertical_body, n_vert=n_vert, per_dev=per_dev, half=half, chunk=chunk),
        grid_spec=pltpu.PrefetchScalarGridSpec(
            num_scalar_prefetch=3,
            grid=(steps,),
            in_specs=[
                q_spec, q_spec,
                pl.BlockSpec((1, rows, dim), lambda h, v, c, place: (at(h, place), 0, 0)),
                whole_spec(tiles),
            ]
            + [pl.BlockSpec(memory_space=pl.ANY)] * len(before),
            out_specs=pl.BlockSpec(
                (rows, PAIR * group, dim), lambda h, v, c, place: (0, at(h, place) // PAIR, 0)
            ),
            scratch_shapes=[
                pltpu.VMEM((n_vert, BLOCK, dim), queries.dtype),
                pltpu.VMEM((n_vert, BLOCK, 2 * dim), queries.dtype),
                pltpu.VMEM((rows * PAIR * group, dim), jnp.float32),
                scores, scores, powers, powers, tops, tops,
            ],
        ),
        out_shape=jax.ShapeDtypeStruct((rows, heads * group, dim), queries.dtype),
        input_output_aliases={7 + i: i for i in range(len(before))},
        cost_estimate=cost(queries, n_vert // 2),
    )(
        verts, vert_count, jnp.stack((device, which)), queries, part, stat, tiles, *before
    )


def local(
    query_states, key_states, value_states, vert_blocks, vert_count, slash_offsets, slash_count
):
    rows_dev, q_heads, head_dim = query_states.shape
    kv_heads = key_states.shape[1]
    group_size = q_heads // kv_heads
    per_dev = rows_dev // BLOCK
    n_vert = vert_blocks.shape[1]
    device = lax.axis_index(ALL).astype(jnp.int32)
    core = device % CORES
    own = jnp.stack((key_states, value_states)).reshape(2, per_dev, BLOCK, kv_heads, head_dim)
    own = jnp.transpose(own, (3, 1, 0, 2, 4)).reshape(kv_heads, per_dev, 2 * BLOCK, head_dim)
    half = kv_heads // 2
    row_end = lax.axis_size("x") - 1
    at_start = lax.axis_index("x") == 0
    low = hop(own[:half], "x", wrap=True)
    low_wrap = hop(low, "y", only=("x", 0))
    high = hop(own[half:], "x")
    high_wrap = hop(own[half:], "y", only=("x", row_end))
    high_wrap = from_last_chip(high_wrap)
    core_kv = lax.ppermute(own, "core", [(0, 1)])
    verts = vert_blocks.reshape(-1)
    slashes = slash_offsets.reshape(-1)
    queries = jnp.moveaxis(query_states.reshape(rows_dev, kv_heads, group_size, head_dim), 0, 2)
    mine, theirs, queries = spread_vertical(
        own.reshape(kv_heads * per_dev, 2 * BLOCK, head_dim),
        verts, vert_count, device, per_dev, n_vert, queries,
    )
    low = jnp.where(at_start, low_wrap, low)
    high = jnp.where(at_start, high_wrap, high)
    low_chip = lax.ppermute(low, "core", [(1, 0)])
    high_chip = lax.ppermute(high, "core", [(1, 0)])
    lists = (verts, vert_count, slashes, slash_count, device)
    state = attend_window(queries, own, core_kv, low_chip, low, (), *lists, 0)
    state = attend_window(queries, own, core_kv, high_chip, high, state, *lists, half // WINDOW)
    lists = (verts, vert_count, device)
    out = attend_vertical(queries, *state, mine, (), *lists, core, per_dev)
    return attend_vertical(queries, *state, theirs, (out,), *lists, 1 - core, per_dev)


def solution(mesh):
    groups, size = mesh.shape["groups"], mesh.shape["ctx"]
    side = math.isqrt(size // CORES)
    parts = Mesh(
        mesh.devices.reshape(groups, size // (CORES * side), side, CORES), ("groups", *ALL)
    )
    rows = P(("groups", *ALL), None, None)
    in_specs = (rows, rows, rows, P("groups", None), P("groups"), P("groups", None), P("groups"))
    return jax.shard_map(local, mesh=parts, in_specs=in_specs, out_specs=rows, check_vma=False)
```
